512 devices in a mesh: grad: 64 (over y_lo, z, core), flow: 8 (over x, y_hi).
Axes of the slice: x: 4, y: 4 (y_hi: 2, y_lo: 2; y = y_hi * 2 + y_lo), z: 16, core: 2. Of those that a mesh axis runs over, the one named last changes fastest.
Arguments:
- bead_pos: float32 [3, 64, 32768], P(None, 'grad', 'flow'), may hold values from 0 to 11, as said below
- bead_vel: float32 [3, 64, 32768], P(None, 'grad', 'flow'), may hold values from -5 to 5
- noise_angle: float32 [2, 64, 32768], P(None, 'grad', 'flow'), may hold values from -3.140625 to 3.140625
- occupancy: int32 [64, 512], P('grad', 'flow'), may hold values from 32 to 64
- image_shift: int32 [1], replicated, may hold values from 0 to 511
- strain: float32 [1], replicated, may hold values from 0.38 to 0.48
Outputs:
- new_pos: float32 [3, 64, 32768], P(None, 'grad', 'flow')
- new_vel: float32 [3, 64, 32768], P(None, 'grad', 'flow')
- stress_profile: float32 [64], P('grad')
The draws below stay inside these ranges and needn't reach their ends.
Inputs may be any that keep to these rules, and one draw needn't show every extreme that they name: `bead_pos`: the first coordinate lies in [0, 2), the second in [0, 1), the third in [0, 64 / 6).
All inputs are finite; a program needn't handle non-finite values.
Results may differ from the reference program's by a relative error of at most 0.0003.
Values sent between devices are 32-bit elements; how exact they have to be, the bound alone decides.
A program may use at most 64 MiB of HBM per device.

```python
import math
import jax
import jax.numpy as jnp
from jax import lax

TB = 64
NX = 512
NY = 64
SLOTS = 32768


def draw_bead_pos(key, part):
    unit = jax.random.uniform(key, (3, NY, NX * TB), jnp.float32)
    scales = jnp.array([2.0, 1.0, TB / 6.0], jnp.float32)[:, None, None]
    return unit * scales


def touch_ends(result, own_key, low, largest):
    longest = result.shape.index(max(result.shape))
    spots = []
    for shift in (0, 1):
        where = [jax.random.randint(jax.random.fold_in(own_key, axis), (), 0, length) for axis, length in enumerate(result.shape)]
        where[longest] = (where[longest] + shift) % result.shape[longest]
        spots.append(tuple(where))
    return result.at[spots[0]].set(low).at[spots[1]].set(largest)


def block_levels(key, dims, split, low, top_value):
    level = 1.0
    for axis_at, shards_of in split:
        draws = jax.random.uniform(jax.random.fold_in(jax.random.fold_in(key, 6), axis_at), (shards_of,), jnp.float32, low / len(split), top_value / len(split))
        level = level * jnp.repeat(jnp.exp(draws), dims[axis_at] // shards_of).reshape((-1,) + (1,) * (len(dims) - 1 - axis_at))
    return level


def scatter_about(key, dims, scale, most, cuts=(), kind=jnp.bfloat16):
    drawn = scale * jax.random.normal(key, dims, jnp.float32)
    if cuts:
        drawn = drawn * block_levels(key, dims, cuts, -0.22, 0.18)
    return jnp.clip(drawn, -most, most).astype(kind)


def setup_inputs(seed: int = 0) -> dict:
    key_of = jax.random.split(jax.random.key(seed), 7)
    bead_pos = draw_bead_pos(jax.random.fold_in(key_of[6], 71), 0)
    bead_vel = scatter_about(key_of[1], (3, NY, SLOTS), 1.0, 5.0, ((1, 64), (2, 8)), jnp.float32)
    noise_angle = jnp.clip(jax.random.uniform(key_of[2], (2, NY, SLOTS), jnp.float32, -3.140625, 3.140625), -3.140625, 3.140625)
    occupancy = touch_ends(jax.random.randint(key_of[3], (NY, NX), TB // 2, TB + 1), jax.random.fold_in(key_of[3], 1), TB // 2, TB).astype(jnp.int32)
    image_shift = jax.random.randint(key_of[4], (1,), 0, NX).astype(jnp.int32)
    strain = jnp.clip(jax.random.uniform(key_of[5], (1,), jnp.float32, 0.38, 0.48), 0.38, 0.48)
    return {"bead_pos": bead_pos, "bead_vel": bead_vel, "noise_angle": noise_angle, "occupancy": occupancy, "image_shift": image_shift, "strain": strain}


repulsion = 25.0
friction = 4.5
noise_gain = 15.0
time_step = 0.04
shear_rate = 0.25
root_two = 1.4142135623730951


def live_slots(occupancy):
    rows_here = occupancy.shape[0]
    width = occupancy.shape[1] * TB
    slot_index = lax.broadcasted_iota(jnp.int32, (rows_here, width), 1) % TB
    limits = jnp.repeat(occupancy, TB, axis=1)
    return (slot_index < limits).astype(jnp.float32)


def band_forces(slab_band, strain_now):
    all_tiles = slab_band.shape[2] // TB
    centre_tiles = all_tiles - 2
    block_tiles = math.gcd(32, centre_tiles)
    tile_grid = slab_band.reshape(slab_band.shape[0], 3, all_tiles, TB)
    box_depth = TB / 6.0
    slot_row = lax.broadcasted_iota(jnp.int32, (TB, 3 * TB), 0)
    slot_col = lax.broadcasted_iota(jnp.int32, (TB, 3 * TB), 1)
    itself = (slot_col == slot_row + TB).astype(jnp.float32)
    offset = jnp.repeat(jnp.array([2.0, 0.0, -2.0], jnp.float32), TB)

    def one_block(first_tile):
        centre = lax.dynamic_slice_in_dim(tile_grid[:, 1], first_tile + 1, block_tiles, 1)[:, :, :, None]
        forces = jnp.zeros((3, block_tiles, TB), jnp.float32)
        virial = jnp.zeros((), jnp.float32)
        for band_row in range(3):
            nearby = lax.dynamic_slice_in_dim(tile_grid[:, band_row], first_tile, block_tiles + 2, 1)
            partners = jnp.concatenate([nearby[:, column:column + block_tiles] for column in range(3)], 2)[:, :, None, :]
            sep_x = centre[0] - partners[0] + offset
            sep_y = centre[1] - partners[1] + (1.0 - band_row)
            sep_z = centre[2] - partners[2]
            sep_z = jnp.where(sep_z > 0.5 * box_depth, sep_z - box_depth, sep_z)
            sep_z = jnp.where(sep_z < -0.5 * box_depth, sep_z + box_depth, sep_z)
            phys_x = sep_x + strain_now * sep_y
            paired = centre[7] * partners[7]
            if band_row == 1:
                paired = paired * (1.0 - itself)
            weight = jnp.maximum(1.0 - phys_x * phys_x - sep_y * sep_y - sep_z * sep_z, 0.0) * paired
            approach = phys_x * (centre[3] - partners[3]) + sep_y * (centre[4] - partners[4]) + sep_z * (centre[5] - partners[5])
            random_kick = root_two * jnp.cos(centre[6] - partners[6])
            magnitude = weight * (repulsion + noise_gain * random_kick - friction * weight * approach)
            forces = forces + jnp.stack([jnp.sum(magnitude * phys_x, -1), jnp.sum(magnitude * sep_y, -1), jnp.sum(magnitude * sep_z, -1)])
            virial = virial + 0.5 * jnp.sum(magnitude * phys_x * sep_y)
        return forces, virial

    starts = jnp.arange(0, centre_tiles, block_tiles, dtype=jnp.int32)
    block_forces, block_virials = lax.map(one_block, starts)
    forces = jnp.transpose(block_forces, (1, 0, 2, 3)).reshape(3, centre_tiles * TB)
    return forces, jnp.sum(block_virials)


def advance(positions, velocity, forces, strain_now):
    vel_x = velocity[0] + time_step * (forces[0] - shear_rate * velocity[1])
    vel_y = velocity[1] + time_step * forces[1]
    vel_z = velocity[2] + time_step * forces[2]
    pos_x = positions[0] + time_step * (vel_x - strain_now * vel_y)
    pos_y = positions[1] + time_step * vel_y
    pos_z = positions[2] + time_step * vel_z
    return jnp.stack([pos_x, pos_y, pos_z]), jnp.stack([vel_x, vel_y, vel_z]), strain_now + shear_rate * time_step


def reference(bead_pos, bead_vel, noise_angle, occupancy, image_shift, strain):
    live_mask = live_slots(occupancy)
    image_tiles = image_shift[0]
    strain_now = strain[0]
    positions, velocity = bead_pos, bead_vel
    running = jnp.zeros((NY,), jnp.float32)
    for step_index in range(2):
        fields = jnp.concatenate([positions, velocity, noise_angle[step_index][None], live_mask[None]], 0)
        below_row = jnp.roll(fields[:, NY - 1], -image_tiles * TB, axis=1)
        above_row = jnp.roll(fields[:, 0], image_tiles * TB, axis=1)
        extended = jnp.concatenate([below_row[:, None], fields, above_row[:, None]], 1)
        extended = jnp.concatenate([extended[:, :, -TB:], extended, extended[:, :, :TB]], 2)

        def one_row(row_index):
            return band_forces(lax.dynamic_slice_in_dim(extended, row_index, 3, 1), strain_now)

        row_forces, virials = lax.map(one_row, jnp.arange(NY, dtype=jnp.int32))
        forces = jnp.transpose(row_forces, (1, 0, 2))
        kinetic = jnp.sum(live_mask * velocity[0] * velocity[1], axis=1)
        running = running + kinetic + virials
        positions, velocity, strain_now = advance(positions, velocity, forces, strain_now)
    row_numbers = jnp.arange(NY, dtype=jnp.int32)
    parity = (row_numbers % 2).astype(jnp.float32)
    shifted_x = positions[0] + parity[:, None] + positions[1]
    stacked = jnp.concatenate([shifted_x[None], positions[1:], velocity], 0)
    remapped = jax.vmap(lambda segment, device_hops: jnp.roll(segment, device_hops * TB, axis=1), in_axes=(1, 0), out_axes=1)(stacked, row_numbers // 2)
    box_depth = TB / 6.0
    stress_profile = (-running / (2.0 * NX * 2.0 * box_depth)).astype(jnp.float32)
    return remapped[:3], remapped[3:], stress_profile
```

```python
import functools

import jax
import jax.numpy as jnp
from jax import lax
from jax.experimental import pallas as pl
from jax.experimental.pallas import tpu as pltpu
from jax.sharding import PartitionSpec as P

TB = 64
LANES = 128
DEPTH = TB / 6.0
INV = 6.0 / TB
REPULSION = 25.0
FRICTION = 4.5
NOISE = 15.0 * 1.4142135623730951
DT = 0.04
RATE = 0.25
FAR = 1.0e6
VSCALE = FRICTION * DEPTH**3
FSCALE = DEPTH**3
WCUT = INV * INV
MESH = pl.DeviceIdType.MESH
f32 = jnp.float32


def body_of(G, F, LP):
    NT = 2 * LP
    NTT = NT * F
    ROWS = 8 * LP
    HP = LP // 2

    def kernel(
        shift_s, strain_s, pos_r, vel_r, cs_r, live_r,
        outp_r, outv_r, stress_r,
        rb, img0, img1, eblk, ecol, jev, jom, jop, facc, fsum, vacc, spos, svel, comb, part,
        ssem, rsem, isend, irecv, fsem, tsend, trecv,
    ):
        g = lax.axis_index("grad")
        f = lax.axis_index("flow")
        up = lax.rem(g + 1, G)
        dn = lax.rem(g + G - 1, G)
        rt = lax.rem(f + 1, F)
        lf = lax.rem(f + F - 1, F)
        first = g == 0
        last = g == G - 1
        img = (img0, img1)
        lane = lax.broadcasted_iota(jnp.int32, (8, LANES), 1)
        sub = lax.broadcasted_iota(jnp.int32, (8, LANES), 0)
        low = lane < TB

        bar = pltpu.get_barrier_semaphore()

        def hello(dg, df):
            pl.semaphore_signal(bar, inc=1, device_id=(dg, df), device_id_type=MESH)

        for k in range(1, F):
            hello(g, lax.rem(f + k, F))

        @pl.when(first)
        def _():
            for k in range(F):
                hello(dn, lax.rem(f + k, F))

        @pl.when(jnp.logical_not(first))
        def _():
            for df in (lf, f, rt):
                hello(dn, df)

        @pl.when(last)
        def _():
            for k in range(F):
                hello(up, lax.rem(f + k, F))

        @pl.when(jnp.logical_not(last))
        def _():
            for df in (lf, f, rt):
                hello(up, df)

        edge = jnp.logical_or(first, last)
        expected = (F - 1) + 6 + jnp.where(edge, F - 3, 0)

        def rcopy(k, ri, pi):
            dg = (up, g, dn)[ri]
            df = (f, rt, lf)[pi]
            src = ((1, LP), (LP, 1), (1, 1))[pi]
            dst = ((1, LP), (0, 1), (LP + 1, 1))[pi]
            return pltpu.make_async_remote_copy(
                src_ref=rb.at[k, 1, pl.ds(*src)],
                dst_ref=rb.at[k, ri, pl.ds(*dst)],
                send_sem=ssem.at[k, ri, pi],
                recv_sem=rsem.at[k, ri, pi],
                device_id=(dg, df),
                device_id_type=MESH,
            )

        def icopy(k, dg, d):
            df = lax.rem(f + d, F)
            return pltpu.make_async_remote_copy(
                src_ref=rb.at[k, 1, pl.ds(1, LP)],
                dst_ref=img[k].at[pl.ds(f * LP, LP)],
                send_sem=isend.at[k, d],
                recv_sem=irecv.at[k, f],
                device_id=(dg, df),
                device_id_type=MESH,
            )

        def iwait(k, d):
            return pltpu.make_async_remote_copy(
                src_ref=rb.at[k, 1, pl.ds(1, LP)],
                dst_ref=img[k].at[pl.ds(d * LP, LP)],
                send_sem=isend.at[k, d],
                recv_sem=irecv.at[k, d],
                device_id=(g, rt),
                device_id_type=MESH,
            )

        def send_rows(k):
            for pi in (1, 2):
                rcopy(k, 1, pi).start()

            @pl.when(first)
            def _():
                for d in range(F):
                    icopy(k, dn, d).start()

            @pl.when(last)
            def _():
                for d in range(F):
                    icopy(k, up, d).start()

            @pl.when(jnp.logical_not(last))
            def _():
                for pi in range(3):
                    rcopy(k, 0, pi).start()

            @pl.when(jnp.logical_not(first))
            def _():
                for pi in range(3):
                    rcopy(k, 2, pi).start()

        def finish_sends(k):
            for pi in (1, 2):
                rcopy(k, 1, pi).wait_send()

            @pl.when(edge)
            def _():
                for d in range(F):
                    icopy(k, dn, d).wait_send()

            @pl.when(jnp.logical_not(last))
            def _():
                for pi in range(3):
                    rcopy(k, 0, pi).wait_send()

            @pl.when(jnp.logical_not(first))
            def _():
                for pi in range(3):
                    rcopy(k, 2, pi).wait_send()

        def write_blocks(k, strain, pos, vel):
            live = live_r[...] > 0.5
            x = (pos[0] + strain * pos[1]) * INV

            def put(field, value):
                rb[k, 1, pl.ds(1, LP), field, :] = value

            def col(field, value):
                eblk[pl.ds(field, LP, stride=8), :] = value

            y, z = pos[1] * INV, pos[2] * INV
            put(0, jnp.where(live, x, FAR))
            col(0, jnp.where(live, x, -FAR))
            put(1, y)
            col(1, y)
            put(2, z)
            col(2, z)
            for i in range(3):
                scaled = vel[i] * VSCALE
                put(3 + i, scaled)
                col(3 + i, scaled)
            cosine, sine = cs_r[2 * k], cs_r[2 * k + 1]
            put(6, cosine)
            col(6, cosine * NOISE)
            put(7, sine)
            col(7, sine * NOISE)

        lane64 = lax.broadcasted_iota(jnp.int32, (TB, LANES), 1)
        low64 = lane64 < TB

        def spread_centres():
            def one(p, carry):
                tile = eblk[pl.ds(pl.multiple_of(p * 8, 8), 8), :]
                turned = tile.T
                for i in range(8):
                    lo = jnp.broadcast_to(turned[:TB, i : i + 1], (TB, LANES))
                    hi = jnp.broadcast_to(turned[TB:, i : i + 1], (TB, LANES))
                    ecol[p, i] = jnp.where(low64, lo, hi)
                return carry

            lax.fori_loop(0, LP, one, 0)

        def offsets(strain, a, b):
            x = (2.0 * b + strain * a) * INV
            y = a * INV
            return jnp.where(sub == 0, x, jnp.where(sub == 1, y, 0.0))

        def halves(left, right):
            return jnp.where(low, pltpu.roll(left, TB, 1), pltpu.roll(right, TB, 1))

        def ready_row(k, ri, strain):
            a = (ri - 1).astype(f32)
            here = offsets(strain, a, 0.0)
            minus = offsets(strain, a, -1.0)
            plus = offsets(strain, a, 1.0)

            def one(q, carry):
                now = rb[k, ri, q]
                nxt = rb[k, ri, q + 1]
                odd = halves(now, nxt)
                at = pl.ds(pl.multiple_of(q * 8, 8), 8)
                jev[at, :] = now + here
                jom[at, :] = odd + minus
                jop[at, :] = odd + plus
                return carry

            lax.fori_loop(0, LP + 1, one, 0)

        def ready_image(k, ri, strain):
            a = (ri - 1).astype(f32)
            here = offsets(strain, a, 0.0)
            minus = offsets(strain, a, -1.0)
            plus = offsets(strain, a, 1.0)
            signed = shift_s[0] * (1 - 2 * lax.div(g, G - 1))

            def one(q, carry):
                tile = lax.rem(NT * f + 2 * q - 2 + signed + 2 * NTT, NTT)
                u = lax.div(tile, 2)
                v = lax.rem(u + 1, NTT // 2)
                one_t = img[k][u]
                two_t = img[k][v]
                mixed = halves(one_t, two_t)
                is_even = jnp.broadcast_to(lax.rem(tile, 2), (8, LANES)) == 0
                now = jnp.where(is_even, one_t, mixed)
                odd = jnp.where(is_even, mixed, two_t)
                at = pl.ds(pl.multiple_of(q * 8, 8), 8)
                jev[at, :] = now + here
                jom[at, :] = odd + minus
                jop[at, :] = odd + plus
                return carry

            lax.fori_loop(0, LP + 1, one, 0)

        def row_pass(k, fresh):
            def one(p, virial):
                def partner(ref, q):
                    base = q * 8
                    return [
                        jnp.broadcast_to(ref[pl.ds(base + i, 1), :], (8, LANES))
                        for i in range(8)
                    ]

                sides = (partner(jom, p), partner(jev, p + 1), partner(jop, p + 1))
                for grp in range(TB // 8):
                    at = pl.ds(grp * 8, 8)
                    ex, ey, ez, eu, ev, ew, ec, es = [ecol[p, i, at, :] for i in range(8)]
                    if fresh:
                        fx = fy = fz = jnp.zeros((8, LANES), f32)
                    else:
                        fx, fy, fz = [facc[p, i, at, :] for i in range(3)]
                    for jx, jy, jz, ju, jv, jw, jc, js in sides:
                        dx = ex - jx
                        dy = ey - jy
                        dz = ez - jz
                        turn = jnp.round(dz)
                        if k > 0:
                            turn = jnp.clip(turn, -1.0, 1.0)
                        dz = dz - turn
                        w = jnp.maximum(WCUT - dx * dx - dy * dy - dz * dz, 0.0)
                        approach = dx * (eu - ju) + dy * (ev - jv) + dz * (ew - jw)
                        kick = REPULSION + (ec * jc + es * js)
                        m = w * (kick - w * approach)
                        mx = m * dx
                        fx = fx + mx
                        fy = fy + m * dy
                        fz = fz + m * dz
                        virial = virial + mx * dy
                    facc[p, 0, at, :] = fx
                    facc[p, 1, at, :] = fy
                    facc[p, 2, at, :] = fz
                return virial

            vacc[...] = lax.fori_loop(0, LP, one, vacc[...])

        def sum_forces():
            for i in range(3):
                fsum[i] = jnp.zeros((TB, LANES), f32)

            def one(p, carry):
                for i in range(3):
                    acc = facc[p, i]
                    lo = jnp.sum(jnp.where(low64, acc, 0.0), axis=1, keepdims=True)
                    hi = jnp.sum(jnp.where(low64, 0.0, acc), axis=1, keepdims=True)
                    now = fsum[i]
                    now = jnp.where(lane64 == p, lo, now)
                    fsum[i] = jnp.where(lane64 == p + LP, hi, now)
                return carry

            lax.fori_loop(0, LP, one, 0)
            forces = []
            lowrow = lax.broadcasted_iota(jnp.int32, (LP, LANES), 1) < TB
            for i in range(3):
                both = jnp.concatenate([fsum[i], fsum[i]], axis=0).T
                forces.append(jnp.where(lowrow, both[:LP], both[LP : 2 * LP]) * FSCALE)
            return forces

        part[F] = jnp.zeros((8, LANES), f32)
        for k in range(2):
            strain = strain_s[0] + k * RATE * DT
            pos = [(pos_r if k == 0 else spos)[i] for i in range(3)]
            vel = [(vel_r if k == 0 else svel)[i] for i in range(3)]
            write_blocks(k, strain, pos, vel)
            if k == 0:
                pl.semaphore_wait(bar, expected)
            send_rows(k)
            spread_centres()
            vacc[...] = jnp.zeros((8, LANES), f32)
            for pi in (1, 2):
                rcopy(k, 1, pi).wait_recv()
            ready_row(k, jnp.int32(1), strain)
            row_pass(k, True)

            @pl.when(jnp.logical_not(first))
            def _():
                for pi in range(3):
                    rcopy(k, 0, pi).wait_recv()
                ready_row(k, jnp.int32(0), strain)

            @pl.when(first)
            def _():
                for pi in range(3):
                    rcopy(k, 2, pi).wait_recv()
                ready_row(k, jnp.int32(2), strain)

            row_pass(k, False)

            @pl.when(jnp.logical_not(edge))
            def _():
                for pi in range(3):
                    rcopy(k, 2, pi).wait_recv()
                ready_row(k, jnp.int32(2), strain)

            @pl.when(edge)
            def _():
                for d in range(F):
                    iwait(k, d).wait_recv()
                ready_image(k, jnp.where(first, 0, 2), strain)

            row_pass(k, False)
            force = sum_forces()
            kinetic = live_r[...] * vel[0] * vel[1]
            folded = kinetic[0:8]
            for q in range(1, LP // 8):
                folded = folded + kinetic[8 * q : 8 * q + 8]
            part[F] = part[F] + folded + vacc[...] * (0.5 * DEPTH**4)
            nvx = vel[0] + DT * (force[0] - RATE * vel[1])
            nvy = vel[1] + DT * force[1]
            nvz = vel[2] + DT * force[2]
            npx = pos[0] + DT * (nvx - strain * nvy)
            npy = pos[1] + DT * nvy
            npz = pos[2] + DT * nvz
            if k == 0:
                for i, value in enumerate((npx, npy, npz)):
                    spos[i] = value
                for i, value in enumerate((nvx, nvy, nvz)):
                    svel[i] = value
            else:
                npx = npx + lax.rem(g, 2).astype(f32) + npy
                for i, value in enumerate((npx, npy, npz, nvx, nvy, nvz)):
                    comb[i, pl.ds(HP, LP), :] = value

        tail = pltpu.make_async_remote_copy(
            src_ref=comb.at[:, pl.ds(LP, HP)],
            dst_ref=comb.at[:, pl.ds(0, HP)],
            send_sem=fsem.at[0],
            recv_sem=fsem.at[1],
            device_id=(g, rt),
            device_id_type=MESH,
        )
        tail.start()

        def share(d):
            return pltpu.make_async_remote_copy(
                src_ref=part.at[F],
                dst_ref=part.at[f],
                send_sem=tsend.at[d],
                recv_sem=trecv.at[f],
                device_id=(g, lax.rem(f + d, F)),
                device_id_type=MESH,
            )

        def shared(d):
            peer = lax.rem(f + d, F)
            return pltpu.make_async_remote_copy(
                src_ref=part.at[F],
                dst_ref=part.at[peer],
                send_sem=tsend.at[d],
                recv_sem=trecv.at[peer],
                device_id=(g, peer),
                device_id_type=MESH,
            )

        for d in range(1, F):
            share(d).start()
        for k in range(2):
            finish_sends(k)
        tail.wait()
        hop = g // 2
        even = lax.rem(hop, 2) == 0
        start = HP - (hop + 1) // 2
        lowrow = lax.broadcasted_iota(jnp.int32, (LP, LANES), 1) < TB

        @pl.when(even)
        def _():
            for i in range(6):
                out = outp_r if i < 3 else outv_r
                out[i % 3] = comb[i, pl.ds(start, LP), :]

        @pl.when(jnp.logical_not(even))
        def _():
            for i in range(6):
                out = outp_r if i < 3 else outv_r
                one = pltpu.roll(comb[i, pl.ds(start, LP), :], TB, 1)
                two = pltpu.roll(comb[i, pl.ds(start + 1, LP), :], TB, 1)
                out[i % 3] = jnp.where(lowrow, one, two)

        total = part[F]
        for d in range(1, F):
            shared(d).wait_recv()
            total = total + part[lax.rem(f + d, F)]
        for d in range(1, F):
            share(d).wait_send()
        whole = jnp.sum(jnp.sum(total, axis=1, keepdims=True), axis=0, keepdims=True)
        stress_r[...] = jnp.broadcast_to(whole * (-1.0 / (2.0 * NTT * 2.0 * DEPTH)), (8, LANES))

    return kernel


def per_device(G, F, bead_pos, bead_vel, noise_angle, occupancy, image_shift, strain):
    width = bead_pos.shape[2]
    LP = width // LANES
    slot = lax.broadcasted_iota(jnp.int32, (1, width), 1) % TB
    live = (slot < jnp.repeat(occupancy, TB, axis=1)).astype(f32).reshape(LP, LANES)
    angle = noise_angle.reshape(2, LP, LANES)
    cs = jnp.stack([jnp.cos(angle), jnp.sin(angle)], 1).reshape(4, LP, LANES)
    vm = pl.BlockSpec(memory_space=pltpu.VMEM)
    sm = pl.BlockSpec(memory_space=pltpu.SMEM)
    rows = 8 * LP
    block = jax.ShapeDtypeStruct((3, LP, LANES), f32)
    dma = pltpu.SemaphoreType.DMA
    newp, newv, stress = pl.pallas_call(
        body_of(G, F, LP),
        out_shape=(block, block, jax.ShapeDtypeStruct((8, LANES), f32)),
        in_specs=[sm, sm, vm, vm, vm, vm],
        out_specs=(vm, vm, vm),
        scratch_shapes=[
            pltpu.VMEM((2, 3, LP + 2, 8, LANES), f32),
            pltpu.VMEM((F * LP, 8, LANES), f32),
            pltpu.VMEM((F * LP, 8, LANES), f32),
            pltpu.VMEM((rows, LANES), f32),
            pltpu.VMEM((LP, 8, TB, LANES), f32),
            pltpu.VMEM((rows + 8, LANES), f32),
            pltpu.VMEM((rows + 8, LANES), f32),
            pltpu.VMEM((rows + 8, LANES), f32),
            pltpu.VMEM((LP, 3, TB, LANES), f32),
            pltpu.VMEM((3, TB, LANES), f32),
            pltpu.VMEM((8, LANES), f32),
            pltpu.VMEM((3, LP, LANES), f32),
            pltpu.VMEM((3, LP, LANES), f32),
            pltpu.VMEM((6, LP + LP // 2, LANES), f32),
            pltpu.VMEM((F + 1, 8, LANES), f32),
            dma((2, 3, 3)),
            dma((2, 3, 3)),
            dma((2, F)),
            dma((2, F)),
            dma((2,)),
            dma((F,)),
            dma((F,)),
        ],
        compiler_params=pltpu.CompilerParams(
            collective_id=0, has_side_effects=True, vmem_limit_bytes=48 * 1024 * 1024
        ),
    )(
        image_shift,
        strain,
        bead_pos.reshape(3, LP, LANES),
        bead_vel.reshape(3, LP, LANES),
        cs,
        live,
    )
    shape = bead_pos.shape
    return newp.reshape(shape), newv.reshape(shape), stress[0, :1]


def solution(mesh):
    G, F = mesh.shape["grad"], mesh.shape["flow"]
    in_specs = (
        P(None, "grad", "flow"),
        P(None, "grad", "flow"),
        P(None, "grad", "flow"),
        P("grad", "flow"),
        P(),
        P(),
    )
    out_specs = (P(None, "grad", "flow"), P(None, "grad", "flow"), P("grad"))
    return jax.shard_map(
        functools.partial(per_device, G, F),
        mesh=mesh,
        in_specs=in_specs,
        out_specs=out_specs,
        check_vma=False,
    )
```

```python
import functools

import jax
import jax.numpy as jnp
from jax import lax
from jax.experimental import pallas as pl
from jax.experimental.pallas import tpu as pltpu
from jax.sharding import PartitionSpec as P

TB = 64
LANES = 128
DEPTH = TB / 6.0
INV = 6.0 / TB
REPULSION = 25.0
FRICTION = 4.5
NOISE = 15.0 * 1.4142135623730951
DT = 0.04
RATE = 0.25
FAR = 1.0e6
TERMS = 48
VSCALE = FRICTION * DEPTH**3
FSCALE = DEPTH**3
WCUT = INV * INV
MESH = pl.DeviceIdType.MESH
f32 = jnp.float32


def body_of(G, F, LP):
    NT = 2 * LP
    NTT = NT * F
    ROWS = 8 * LP
    HP = LP // 2

    def kernel(
        shift_s, strain_s, pos_r, vel_r, angle_r, occ_r,
        outp_r, outv_r, stress_r,
        rb, img0, img1, eblk, weights, live_v, cs_v, ecol, jev, jom, jop, facc, picks, vacc, spos, svel, comb, part,
        ssem, rsem, isend, irecv, fsem, tsend, trecv,
    ):
        g = lax.axis_index("grad")
        f = lax.axis_index("flow")
        up = lax.rem(g + 1, G)
        dn = lax.rem(g + G - 1, G)
        rt = lax.rem(f + 1, F)
        lf = lax.rem(f + F - 1, F)
        first = g == 0
        last = g == G - 1
        img = (img0, img1)
        lane = lax.broadcasted_iota(jnp.int32, (8, LANES), 1)
        sub = lax.broadcasted_iota(jnp.int32, (8, LANES), 0)
        low = lane < TB

        bar = pltpu.get_barrier_semaphore()

        def hello(dg, df):
            pl.semaphore_signal(bar, inc=1, device_id=(dg, df), device_id_type=MESH)

        for k in range(1, F):
            hello(g, lax.rem(f + k, F))

        @pl.when(first)
        def _():
            for k in range(F):
                hello(dn, lax.rem(f + k, F))

        @pl.when(jnp.logical_not(first))
        def _():
            for df in (lf, f, rt):
                hello(dn, df)

        @pl.when(last)
        def _():
            for k in range(F):
                hello(up, lax.rem(f + k, F))

        @pl.when(jnp.logical_not(last))
        def _():
            for df in (lf, f, rt):
                hello(up, df)

        edge = jnp.logical_or(first, last)
        expected = (F - 1) + 6 + jnp.where(edge, F - 3, 0)

        def rcopy(k, ri, pi):
            dg = (up, g, dn)[ri]
            df = (f, rt, lf)[pi]
            src = ((1, LP), (LP, 1), (1, 1))[pi]
            dst = ((1, LP), (0, 1), (LP + 1, 1))[pi]
            return pltpu.make_async_remote_copy(
                src_ref=rb.at[k, 1, pl.ds(*src)],
                dst_ref=rb.at[k, ri, pl.ds(*dst)],
                send_sem=ssem.at[k, ri, pi],
                recv_sem=rsem.at[k, ri, pi],
                device_id=(dg, df),
                device_id_type=MESH,
            )

        def icopy(k, dg, d):
            df = lax.rem(f + d, F)
            return pltpu.make_async_remote_copy(
                src_ref=rb.at[k, 1, pl.ds(1, LP)],
                dst_ref=img[k].at[pl.ds(f * LP, LP)],
                send_sem=isend.at[k, d],
                recv_sem=irecv.at[k, f],
                device_id=(dg, df),
                device_id_type=MESH,
            )

        def iwait(k, d):
            return pltpu.make_async_remote_copy(
                src_ref=rb.at[k, 1, pl.ds(1, LP)],
                dst_ref=img[k].at[pl.ds(d * LP, LP)],
                send_sem=isend.at[k, d],
                recv_sem=irecv.at[k, d],
                device_id=(g, rt),
                device_id_type=MESH,
            )

        def send_rows(k):
            for pi in (1, 2):
                rcopy(k, 1, pi).start()

            @pl.when(first)
            def _():
                for d in range(F):
                    icopy(k, dn, d).start()

            @pl.when(last)
            def _():
                for d in range(F):
                    icopy(k, up, d).start()

            @pl.when(jnp.logical_not(last))
            def _():
                for pi in range(3):
                    rcopy(k, 0, pi).start()

            @pl.when(jnp.logical_not(first))
            def _():
                for pi in range(3):
                    rcopy(k, 2, pi).start()

        def finish_sends(k):
            for pi in (1, 2):
                rcopy(k, 1, pi).wait_send()

            @pl.when(edge)
            def _():
                for d in range(F):
                    icopy(k, dn, d).wait_send()

            @pl.when(jnp.logical_not(last))
            def _():
                for pi in range(3):
                    rcopy(k, 0, pi).wait_send()

            @pl.when(jnp.logical_not(first))
            def _():
                for pi in range(3):
                    rcopy(k, 2, pi).wait_send()

        def write_blocks(k, strain, pos, vel):
            live = live_v[...] > 0.5
            x = (pos[0] + strain * pos[1]) * INV

            def put(field, value):
                rb[k, 1, pl.ds(1, LP), field, :] = value

            def col(field, value):
                rest = value
                for term in range(3):
                    piece = rest.astype(jnp.bfloat16).astype(f32)
                    rest = rest - piece
                    for half in range(2):
                        turned = pltpu.roll(piece, TB, 1) if half else piece
                        eblk[pl.ds(term * 16 + half * 8 + field, LP, stride=TERMS), :] = turned

            y, z = pos[1] * INV, pos[2] * INV
            cosine, sine = cs_v[2 * k], cs_v[2 * k + 1]
            scaled = [vel[i] * VSCALE for i in range(3)]
            for field, value in enumerate((jnp.where(live, x, FAR), y, z, *scaled, cosine, sine)):
                put(field, value)

            def columns():
                left = (jnp.where(live, x, -FAR), y, z, *scaled, cosine * NOISE, sine * NOISE)
                for field, value in enumerate(left):
                    col(field, value)

            return columns

        def fill_weights():
            row = lax.broadcasted_iota(jnp.int32, (TERMS, 8 * LANES), 0)
            column = lax.broadcasted_iota(jnp.int32, (TERMS, 8 * LANES), 1)
            same = lax.rem(row, 16) == lax.rem(column // TB, 2) * 8 + column // LANES
            weights[...] = same.astype(f32).astype(jnp.bfloat16)

        def spread_centres():
            step = 4 if LP % 4 == 0 else 1

            def some(c, carry):
                turned = []
                for j in range(step):
                    at = pl.ds(pl.multiple_of((c * step + j) * TERMS, TERMS), TERMS)
                    turned.append(eblk[at, :].T[:TB].astype(jnp.bfloat16))
                for j in range(step):
                    ecol[c * step + j] = jnp.dot(
                        turned[j], weights[...], preferred_element_type=f32
                    )
                return carry

            lax.fori_loop(0, LP // step, some, 0)

        def offsets(strain, a, b):
            x = (2.0 * b + strain * a) * INV
            y = a * INV
            return jnp.where(sub == 0, x, jnp.where(sub == 1, y, 0.0))

        def halves(left, right):
            return jnp.where(low, pltpu.roll(left, TB, 1), pltpu.roll(right, TB, 1))

        def several(one):
            step = 11 if (LP + 1) % 11 == 0 else 1

            def some(c, carry):
                for j in range(step):
                    one(c * step + j)
                return carry

            lax.fori_loop(0, (LP + 1) // step, some, 0)

        def ready_row(k, ri, strain):
            a = (ri - 1).astype(f32)
            here = offsets(strain, a, 0.0)
            minus = offsets(strain, a, -1.0)
            plus = offsets(strain, a, 1.0)

            def one(q):
                now = rb[k, ri, q]
                nxt = rb[k, ri, q + 1]
                odd = halves(now, nxt)
                at = pl.ds(pl.multiple_of(q * 8, 8), 8)
                jev[at, :] = now + here
                jom[at, :] = odd + minus
                jop[at, :] = odd + plus

            several(one)

        def ready_image(k, ri, strain):
            a = (ri - 1).astype(f32)
            here = offsets(strain, a, 0.0)
            minus = offsets(strain, a, -1.0)
            plus = offsets(strain, a, 1.0)
            signed = shift_s[0] * (1 - 2 * lax.div(g, G - 1))

            def one(q):
                tile = lax.rem(NT * f + 2 * q - 2 + signed + 2 * NTT, NTT)
                u = lax.div(tile, 2)
                v = lax.rem(u + 1, NTT // 2)
                one_t = img[k][u]
                two_t = img[k][v]
                mixed = halves(one_t, two_t)
                is_even = jnp.broadcast_to(lax.rem(tile, 2), (8, LANES)) == 0
                now = jnp.where(is_even, one_t, mixed)
                odd = jnp.where(is_even, mixed, two_t)
                at = pl.ds(pl.multiple_of(q * 8, 8), 8)
                jev[at, :] = now + here
                jom[at, :] = odd + minus
                jop[at, :] = odd + plus

            several(one)

        def row_pass(k, fresh):
            def one(p, virial):
                def partner(ref, q):
                    base = q * 8
                    return [
                        jnp.broadcast_to(ref[pl.ds(base + i, 1), :], (8, LANES))
                        for i in range(8)
                    ]

                wide = pl.ds(pl.multiple_of(p * LANES, LANES), LANES)
                sides = (partner(jom, p), partner(jev, p + 1), partner(jop, p + 1))
                for grp in range(TB // 8):
                    at = pl.ds(grp * 8, 8)
                    ex, ey, ez, eu, ev, ew, ec, es = [ecol[p, at, pl.ds(i * LANES, LANES)] for i in range(8)]
                    if fresh:
                        fx = fy = fz = jnp.zeros((8, LANES), f32)
                    else:
                        fx, fy, fz = [facc[pl.ds(i * TB + grp * 8, 8), wide] for i in range(3)]
                    for jx, jy, jz, ju, jv, jw, jc, js in sides:
                        dx = ex - jx
                        dy = ey - jy
                        dz = ez - jz
                        turn = jnp.round(dz)
                        if k > 0:
                            turn = jnp.clip(turn, -1.0, 1.0)
                        dz = dz - turn
                        w = jnp.maximum(WCUT - dx * dx - dy * dy - dz * dz, 0.0)
                        approach = dx * (eu - ju) + dy * (ev - jv) + dz * (ew - jw)
                        kick = REPULSION + (ec * jc + es * js)
                        m = w * (kick - w * approach)
                        mx = m * dx
                        fx = fx + mx
                        fy = fy + m * dy
                        fz = fz + m * dz
                        virial = virial + mx * dy
                    facc[pl.ds(0 * TB + grp * 8, 8), wide] = fx
                    facc[pl.ds(1 * TB + grp * 8, 8), wide] = fy
                    facc[pl.ds(2 * TB + grp * 8, 8), wide] = fz
                return virial

            vacc[...] = lax.fori_loop(0, LP, one, vacc[...])

        lowrow = lax.broadcasted_iota(jnp.int32, (LP, LANES), 1) < TB

        def fill_picks():
            tile = lax.broadcasted_iota(jnp.int32, (LANES, LANES), 0) // TB * LP
            column = lax.broadcasted_iota(jnp.int32, (LANES, LANES), 1) - tile

            def one(p, carry):
                at = pl.ds(pl.multiple_of(p * LANES, LANES), LANES)
                picks[at, :] = (column == p).astype(f32).astype(jnp.bfloat16)
                return carry

            lax.fori_loop(0, LP, one, 0)

        def sum_forces():
            acc = facc[...]
            big = acc.astype(jnp.bfloat16)
            small = (acc - big.astype(f32)).astype(jnp.bfloat16)
            pick = picks[...]
            summed = jnp.dot(big, pick, preferred_element_type=f32)
            summed = summed + jnp.dot(small, pick, preferred_element_type=f32)
            forces = []
            for i in range(3):
                part_i = summed[i * TB : (i + 1) * TB]
                both = jnp.concatenate([part_i, part_i], axis=0).T
                forces.append(jnp.where(lowrow, both[:LP], both[LP : 2 * LP]) * FSCALE)
            return forces

        part[F] = jnp.zeros((8, LANES), f32)
        tile_of = lax.broadcasted_iota(jnp.int32, (LP, NT), 1)
        row_of = lax.broadcasted_iota(jnp.int32, (LP, NT), 0)
        counts = jnp.broadcast_to(occ_r[...].astype(f32), (LP, NT))
        counts = jnp.where(tile_of // 2 == row_of, counts, 0.0).astype(jnp.bfloat16)
        side = lax.rem(lax.broadcasted_iota(jnp.int32, (NT, LANES), 0), 2)
        half = lax.broadcasted_iota(jnp.int32, (NT, LANES), 1) // TB
        limit = jnp.dot(
            counts, (side == half).astype(f32).astype(jnp.bfloat16), preferred_element_type=f32
        )
        slot = lax.rem(lax.broadcasted_iota(jnp.int32, (LP, LANES), 1), TB).astype(f32)
        live_v[...] = (slot < limit).astype(f32)
        cs_v[0] = jnp.cos(angle_r[0])
        cs_v[1] = jnp.sin(angle_r[0])
        for k in range(2):
            strain = strain_s[0] + k * RATE * DT
            pos = [(pos_r if k == 0 else spos)[i] for i in range(3)]
            vel = [(vel_r if k == 0 else svel)[i] for i in range(3)]
            columns = write_blocks(k, strain, pos, vel)
            if k == 0:
                pl.semaphore_wait(bar, expected)
            send_rows(k)
            if k == 0:
                cs_v[2] = jnp.cos(angle_r[1])
                cs_v[3] = jnp.sin(angle_r[1])
                fill_picks()
                fill_weights()
            columns()
            spread_centres()
            vacc[...] = jnp.zeros((8, LANES), f32)
            for pi in (1, 2):
                rcopy(k, 1, pi).wait_recv()
            ready_row(k, jnp.int32(1), strain)
            row_pass(k, True)

            @pl.when(jnp.logical_not(first))
            def _():
                for pi in range(3):
                    rcopy(k, 0, pi).wait_recv()

            @pl.when(first)
            def _():
                for pi in range(3):
                    rcopy(k, 2, pi).wait_recv()

            ready_row(k, jnp.where(first, 2, 0), strain)
            row_pass(k, False)

            @pl.when(jnp.logical_not(edge))
            def _():
                for pi in range(3):
                    rcopy(k, 2, pi).wait_recv()
                ready_row(k, jnp.int32(2), strain)

            @pl.when(edge)
            def _():
                for d in range(F):
                    iwait(k, d).wait_recv()
                ready_image(k, jnp.where(first, 0, 2), strain)

            row_pass(k, False)
            force = sum_forces()
            kinetic = live_v[...] * vel[0] * vel[1]
            folded = kinetic[0:8]
            for q in range(1, LP // 8):
                folded = folded + kinetic[8 * q : 8 * q + 8]
            part[F] = part[F] + folded + vacc[...] * (0.5 * DEPTH**4)
            nvx = vel[0] + DT * (force[0] - RATE * vel[1])
            nvy = vel[1] + DT * force[1]
            nvz = vel[2] + DT * force[2]
            npx = pos[0] + DT * (nvx - strain * nvy)
            npy = pos[1] + DT * nvy
            npz = pos[2] + DT * nvz
            if k == 0:
                for i, value in enumerate((npx, npy, npz)):
                    spos[i] = value
                for i, value in enumerate((nvx, nvy, nvz)):
                    svel[i] = value
            else:
                npx = npx + lax.rem(g, 2).astype(f32) + npy
                for i, value in enumerate((npx, npy, npz, nvx, nvy, nvz)):
                    comb[i, pl.ds(HP, LP), :] = value

        tail = pltpu.make_async_remote_copy(
            src_ref=comb.at[:, pl.ds(LP, HP)],
            dst_ref=comb.at[:, pl.ds(0, HP)],
            send_sem=fsem.at[0],
            recv_sem=fsem.at[1],
            device_id=(g, rt),
            device_id_type=MESH,
        )
        tail.start()

        def share(d):
            return pltpu.make_async_remote_copy(
                src_ref=part.at[F],
                dst_ref=part.at[f],
                send_sem=tsend.at[d],
                recv_sem=trecv.at[f],
                device_id=(g, lax.rem(f + d, F)),
                device_id_type=MESH,
            )

        def shared(d):
            peer = lax.rem(f + d, F)
            return pltpu.make_async_remote_copy(
                src_ref=part.at[F],
                dst_ref=part.at[peer],
                send_sem=tsend.at[d],
                recv_sem=trecv.at[peer],
                device_id=(g, peer),
                device_id_type=MESH,
            )

        for d in range(1, F):
            share(d).start()
        for k in range(2):
            finish_sends(k)
        tail.wait()
        hop = g // 2
        even = lax.rem(hop, 2) == 0
        start = HP - (hop + 1) // 2

        @pl.when(even)
        def _():
            for i in range(6):
                out = outp_r if i < 3 else outv_r
                out[i % 3] = comb[i, pl.ds(start, LP), :]

        @pl.when(jnp.logical_not(even))
        def _():
            for i in range(6):
                out = outp_r if i < 3 else outv_r
                one = pltpu.roll(comb[i, pl.ds(start, LP), :], TB, 1)
                two = pltpu.roll(comb[i, pl.ds(start + 1, LP), :], TB, 1)
                out[i % 3] = jnp.where(lowrow, one, two)

        total = part[F]
        for d in range(1, F):
            shared(d).wait_recv()
            total = total + part[lax.rem(f + d, F)]
        for d in range(1, F):
            share(d).wait_send()
        whole = jnp.sum(jnp.sum(total, axis=1, keepdims=True), axis=0, keepdims=True)
        stress_r[...] = jnp.broadcast_to(whole * (-1.0 / (2.0 * NTT * 2.0 * DEPTH)), (8, LANES))

    return kernel


def per_device(G, F, bead_pos, bead_vel, noise_angle, occupancy, image_shift, strain):
    width = bead_pos.shape[2]
    LP = width // LANES
    vm = pl.BlockSpec(memory_space=pltpu.VMEM)
    sm = pl.BlockSpec(memory_space=pltpu.SMEM)
    rows = 8 * LP
    block = jax.ShapeDtypeStruct((3, LP, LANES), f32)
    dma = pltpu.SemaphoreType.DMA
    newp, newv, stress = pl.pallas_call(
        body_of(G, F, LP),
        out_shape=(block, block, jax.ShapeDtypeStruct((8, LANES), f32)),
        in_specs=[sm, sm, vm, vm, vm, vm],
        out_specs=(vm, vm, vm),
        scratch_shapes=[
            pltpu.VMEM((2, 3, LP + 2, 8, LANES), f32),
            pltpu.VMEM((F * LP, 8, LANES), f32),
            pltpu.VMEM((F * LP, 8, LANES), f32),
            pltpu.VMEM((LP * TERMS, LANES), f32),
            pltpu.VMEM((TERMS, 8 * LANES), jnp.bfloat16),
            pltpu.VMEM((LP, LANES), f32),
            pltpu.VMEM((4, LP, LANES), f32),
            pltpu.VMEM((LP, TB, 8 * LANES), f32),
            pltpu.VMEM((rows + 8, LANES), f32),
            pltpu.VMEM((rows + 8, LANES), f32),
            pltpu.VMEM((rows + 8, LANES), f32),
            pltpu.VMEM((3 * TB, LP * LANES), f32),
            pltpu.VMEM((LP * LANES, LANES), jnp.bfloat16),
            pltpu.VMEM((8, LANES), f32),
            pltpu.VMEM((3, LP, LANES), f32),
            pltpu.VMEM((3, LP, LANES), f32),
            pltpu.VMEM((6, LP + LP // 2, LANES), f32),
            pltpu.VMEM((F + 1, 8, LANES), f32),
            dma((2, 3, 3)),
            dma((2, 3, 3)),
            dma((2, F)),
            dma((2, F)),
            dma((2,)),
            dma((F,)),
            dma((F,)),
        ],
        compiler_params=pltpu.CompilerParams(
            collective_id=0, has_side_effects=True, vmem_limit_bytes=48 * 1024 * 1024
        ),
    )(
        image_shift,
        strain,
        bead_pos.reshape(3, LP, LANES),
        bead_vel.reshape(3, LP, LANES),
        noise_angle.reshape(2, LP, LANES),
        occupancy,
    )
    shape = bead_pos.shape
    return newp.reshape(shape), newv.reshape(shape), stress[0, :1]


def solution(mesh):
    G, F = mesh.shape["grad"], mesh.shape["flow"]
    in_specs = (
        P(None, "grad", "flow"),
        P(None, "grad", "flow"),
        P(None, "grad", "flow"),
        P("grad", "flow"),
        P(),
        P(),
    )
    out_specs = (P(None, "grad", "flow"), P(None, "grad", "flow"), P("grad"))
    return jax.shard_map(
        functools.partial(per_device, G, F),
        mesh=mesh,
        in_specs=in_specs,
        out_specs=out_specs,
        check_vma=False,
    )
```

```python
import functools

import jax
import jax.numpy as jnp
from jax import lax
from jax.experimental import pallas as pl
from jax.experimental.pallas import tpu as pltpu
from jax.sharding import PartitionSpec as P

TB = 64
LANES = 128
DEPTH = TB / 6.0
INV = 6.0 / TB
REPULSION = 25.0
FRICTION = 4.5
NOISE = 15.0 * 1.4142135623730951
DT = 0.04
RATE = 0.25
FAR = 1.0e6
TERMS = 48
SPAN = 4
VSCALE = FRICTION * DEPTH**3
FSCALE = DEPTH**3
WCUT = INV * INV
MESH = pl.DeviceIdType.MESH
f32 = jnp.float32


def body_of(G, F, LP, QLO, NQ):
    NT = 2 * LP
    NTT = NT * F
    ROWS = 8 * LP
    HP = LP // 2

    def kernel(
        shift_s, strain_s, pos_r, vel_r, angle_r, occ_r,
        outp_r, outv_r, stress_r,
        rb, img0, img1, eblk, weights, live_v, cs_v, ecol, jev, jom, jop, facc, picks, vacc, spos, svel, comb, part,
        ssem, rsem, isend, irecv, fsem, tsend, trecv,
    ):
        g = lax.axis_index("grad")
        f = lax.axis_index("flow")
        up = lax.rem(g + 1, G)
        dn = lax.rem(g + G - 1, G)
        rt = lax.rem(f + 1, F)
        lf = lax.rem(f + F - 1, F)
        first = g == 0
        last = g == G - 1
        img = (img0, img1)
        lane = lax.broadcasted_iota(jnp.int32, (8, LANES), 1)
        sub = lax.broadcasted_iota(jnp.int32, (8, LANES), 0)
        low = lane < TB

        bar = pltpu.get_barrier_semaphore()

        def hello(dg, df):
            pl.semaphore_signal(bar, inc=1, device_id=(dg, df), device_id_type=MESH)

        for k in range(1, F):
            hello(g, lax.rem(f + k, F))

        @pl.when(first)
        def _():
            for k in range(F):
                hello(dn, lax.rem(f + k, F))

        @pl.when(jnp.logical_not(first))
        def _():
            for df in (lf, f, rt):
                hello(dn, df)

        @pl.when(last)
        def _():
            for k in range(F):
                hello(up, lax.rem(f + k, F))

        @pl.when(jnp.logical_not(last))
        def _():
            for df in (lf, f, rt):
                hello(up, df)

        edge = jnp.logical_or(first, last)
        expected = (F - 1) + 6 + jnp.where(edge, F - 3, 0)

        def rcopy(k, ri, pi):
            dg = (up, g, dn)[ri]
            df = (f, rt, lf)[pi]
            src = ((1, LP), (LP, 1), (1, 1))[pi]
            dst = ((1, LP), (0, 1), (LP + 1, 1))[pi]
            return pltpu.make_async_remote_copy(
                src_ref=rb.at[k, 1, pl.ds(*src)],
                dst_ref=rb.at[k, ri, pl.ds(*dst)],
                send_sem=ssem.at[k, ri, pi],
                recv_sem=rsem.at[k, ri, pi],
                device_id=(dg, df),
                device_id_type=MESH,
            )

        offs = [(d, d < 0) for d in range(-1, NQ + 1)]

        def icopy(k, d):
            hop = QLO + offs[d][0]
            df = lax.rem(f + jnp.where(first, hop, -hop) + 2 * F, F)
            dg = jnp.where(first, dn, up)
            if offs[d][1]:
                at = jnp.where(first, 0, LP - 1)
                count = 1
            else:
                at, count = 0, LP
            return pltpu.make_async_remote_copy(
                src_ref=rb.at[k, 1, pl.ds(1 + at, count)],
                dst_ref=img[k].at[pl.ds(f * LP + at, count)],
                send_sem=isend.at[k, d],
                recv_sem=irecv.at[k, d],
                device_id=(dg, df),
                device_id_type=MESH,
            )

        def iwait(k, d):
            hop = QLO + offs[d][0]
            df = lax.rem(f + jnp.where(first, hop, -hop) + 2 * F, F)
            dg = jnp.where(first, dn, up)
            if offs[d][1]:
                at = jnp.where(first, LP - 1, 0)
                count = 1
            else:
                at, count = 0, LP
            return pltpu.make_async_remote_copy(
                src_ref=rb.at[k, 1, pl.ds(1 + at, count)],
                dst_ref=img[k].at[pl.ds(df * LP + at, count)],
                send_sem=isend.at[k, d],
                recv_sem=irecv.at[k, d],
                device_id=(dg, df),
                device_id_type=MESH,
            )

        def send_rows(k):
            for pi in (1, 2):
                rcopy(k, 1, pi).start()

            @pl.when(edge)
            def _():
                for d in range(NQ + 2):
                    icopy(k, d).start()

            @pl.when(jnp.logical_not(last))
            def _():
                for pi in range(3):
                    rcopy(k, 0, pi).start()

            @pl.when(jnp.logical_not(first))
            def _():
                for pi in range(3):
                    rcopy(k, 2, pi).start()

        def finish_sends(k):
            for pi in (1, 2):
                rcopy(k, 1, pi).wait_send()

            @pl.when(edge)
            def _():
                for d in range(NQ + 2):
                    icopy(k, d).wait_send()

            @pl.when(jnp.logical_not(last))
            def _():
                for pi in range(3):
                    rcopy(k, 0, pi).wait_send()

            @pl.when(jnp.logical_not(first))
            def _():
                for pi in range(3):
                    rcopy(k, 2, pi).wait_send()

        def write_blocks(k, strain, pos, vel):
            live = live_v[...] > 0.5
            x = (pos[0] + strain * pos[1]) * INV

            def put(field, value):
                rb[k, 1, pl.ds(1, LP), field, :] = value

            def col(field, value):
                rest = value
                for term in range(3):
                    piece = rest.astype(jnp.bfloat16).astype(f32)
                    rest = rest - piece
                    for half in range(2):
                        turned = pltpu.roll(piece, TB, 1) if half else piece
                        eblk[pl.ds(term * 16 + half * 8 + field, LP, stride=TERMS), :] = turned

            y, z = pos[1] * INV, pos[2] * INV
            cosine, sine = cs_v[2 * k], cs_v[2 * k + 1]
            scaled = [vel[i] * VSCALE for i in range(3)]
            for field, value in enumerate((jnp.where(live, x, FAR), y, z, *scaled, cosine, sine)):
                put(field, value)

            def columns():
                left = (jnp.where(live, x, -FAR), y, z, *scaled, cosine * NOISE, sine * NOISE)
                for field, value in enumerate(left):
                    col(field, value)

            return columns

        def fill_weights():
            row = lax.broadcasted_iota(jnp.int32, (TERMS, 8 * LANES), 0)
            column = lax.broadcasted_iota(jnp.int32, (TERMS, 8 * LANES), 1)
            same = lax.rem(row, 16) == lax.rem(column // TB, 2) * 8 + column // LANES
            weights[...] = same.astype(f32).astype(jnp.bfloat16)

        def spread_centres():
            step = 4 if LP % 4 == 0 else 1

            def some(c, carry):
                turned = []
                for j in range(step):
                    at = pl.ds(pl.multiple_of((c * step + j) * TERMS, TERMS), TERMS)
                    turned.append(eblk[at, :].T[:TB].astype(jnp.bfloat16))
                for j in range(step):
                    ecol[c * step + j] = jnp.dot(
                        turned[j], weights[...], preferred_element_type=f32
                    )
                return carry

            lax.fori_loop(0, LP // step, some, 0)

        def offsets(strain, a, b):
            x = (2.0 * b + strain * a) * INV
            y = a * INV
            return jnp.where(sub == 0, x, jnp.where(sub == 1, y, 0.0))

        def halves(left, right):
            return jnp.where(low, pltpu.roll(left, TB, 1), pltpu.roll(right, TB, 1))

        def several(one):
            step = 11 if (LP + 1) % 11 == 0 else 1

            def some(c, carry):
                for j in range(step):
                    one(c * step + j)
                return carry

            lax.fori_loop(0, (LP + 1) // step, some, 0)

        def ready_row(k, ri, strain):
            a = (ri - 1).astype(f32)
            here = offsets(strain, a, 0.0)
            minus = offsets(strain, a, -1.0)
            plus = offsets(strain, a, 1.0)

            def one(q):
                now = rb[k, ri, q]
                nxt = rb[k, ri, q + 1]
                odd = halves(now, nxt)
                at = pl.ds(pl.multiple_of(q * 8, 8), 8)
                jev[at, :] = now + here
                jom[at, :] = odd + minus
                jop[at, :] = odd + plus

            several(one)

        def ready_image(k, ri, strain):
            a = (ri - 1).astype(f32)
            here = offsets(strain, a, 0.0)
            minus = offsets(strain, a, -1.0)
            plus = offsets(strain, a, 1.0)
            signed = shift_s[0] * (1 - 2 * lax.div(g, G - 1))

            def one(q):
                tile = lax.rem(NT * f + 2 * q - 2 + signed + 2 * NTT, NTT)
                u = lax.div(tile, 2)
                v = lax.rem(u + 1, NTT // 2)
                one_t = img[k][u]
                two_t = img[k][v]
                mixed = halves(one_t, two_t)
                is_even = jnp.broadcast_to(lax.rem(tile, 2), (8, LANES)) == 0
                now = jnp.where(is_even, one_t, mixed)
                odd = jnp.where(is_even, mixed, two_t)
                at = pl.ds(pl.multiple_of(q * 8, 8), 8)
                jev[at, :] = now + here
                jom[at, :] = odd + minus
                jop[at, :] = odd + plus

            several(one)

        def row_pass(k, fresh):
            def one(p, virial):
                def partner(ref, q):
                    base = q * 8
                    return [
                        jnp.broadcast_to(ref[pl.ds(base + i, 1), :], (8, LANES))
                        for i in range(8)
                    ]

                wide = pl.ds(pl.multiple_of(p * LANES, LANES), LANES)
                sides = (partner(jom, p), partner(jev, p + 1), partner(jop, p + 1))
                for grp in range(TB // 8):
                    at = pl.ds(grp * 8, 8)
                    ex, ey, ez, eu, ev, ew, ec, es = [ecol[p, at, pl.ds(i * LANES, LANES)] for i in range(8)]
                    if fresh:
                        fx = fy = fz = jnp.zeros((8, LANES), f32)
                    else:
                        fx, fy, fz = [facc[pl.ds(i * TB + grp * 8, 8), wide] for i in range(3)]
                    for jx, jy, jz, ju, jv, jw, jc, js in sides:
                        dx = ex - jx
                        dy = ey - jy
                        dz = ez - jz
                        turn = jnp.round(dz)
                        if k > 0:
                            turn = jnp.clip(turn, -1.0, 1.0)
                        dz = dz - turn
                        w = jnp.maximum(WCUT - dx * dx - dy * dy - dz * dz, 0.0)
                        approach = dx * (eu - ju) + dy * (ev - jv) + dz * (ew - jw)
                        kick = REPULSION + (ec * jc + es * js)
                        m = w * (kick - w * approach)
                        mx = m * dx
                        fx = fx + mx
                        fy = fy + m * dy
                        fz = fz + m * dz
                        virial = virial + mx * dy
                    facc[pl.ds(0 * TB + grp * 8, 8), wide] = fx
                    facc[pl.ds(1 * TB + grp * 8, 8), wide] = fy
                    facc[pl.ds(2 * TB + grp * 8, 8), wide] = fz
                return virial

            vacc[...] = lax.fori_loop(0, LP, one, vacc[...])

        lowrow = lax.broadcasted_iota(jnp.int32, (LP, LANES), 1) < TB

        def fill_picks():
            tile = lax.broadcasted_iota(jnp.int32, (LANES, LANES), 0) // TB * LP
            column = lax.broadcasted_iota(jnp.int32, (LANES, LANES), 1) - tile

            def one(p, carry):
                at = pl.ds(pl.multiple_of(p * LANES, LANES), LANES)
                picks[at, :] = (column == p).astype(f32).astype(jnp.bfloat16)
                return carry

            lax.fori_loop(0, LP, one, 0)

        def sum_forces():
            acc = facc[...]
            big = acc.astype(jnp.bfloat16)
            small = (acc - big.astype(f32)).astype(jnp.bfloat16)
            pick = picks[...]
            summed = jnp.dot(big, pick, preferred_element_type=f32)
            summed = summed + jnp.dot(small, pick, preferred_element_type=f32)
            forces = []
            for i in range(3):
                part_i = summed[i * TB : (i + 1) * TB]
                both = jnp.concatenate([part_i, part_i], axis=0).T
                forces.append(jnp.where(lowrow, both[:LP], both[LP : 2 * LP]) * FSCALE)
            return forces

        part[F] = jnp.zeros((8, LANES), f32)
        tile_of = lax.broadcasted_iota(jnp.int32, (LP, NT), 1)
        row_of = lax.broadcasted_iota(jnp.int32, (LP, NT), 0)
        counts = jnp.broadcast_to(occ_r[...].astype(f32), (LP, NT))
        counts = jnp.where(tile_of // 2 == row_of, counts, 0.0).astype(jnp.bfloat16)
        side = lax.rem(lax.broadcasted_iota(jnp.int32, (NT, LANES), 0), 2)
        half = lax.broadcasted_iota(jnp.int32, (NT, LANES), 1) // TB
        limit = jnp.dot(
            counts, (side == half).astype(f32).astype(jnp.bfloat16), preferred_element_type=f32
        )
        slot = lax.rem(lax.broadcasted_iota(jnp.int32, (LP, LANES), 1), TB).astype(f32)
        live_v[...] = (slot < limit).astype(f32)
        cs_v[0] = jnp.cos(angle_r[0])
        cs_v[1] = jnp.sin(angle_r[0])
        for k in range(2):
            strain = strain_s[0] + k * RATE * DT
            pos = [(pos_r if k == 0 else spos)[i] for i in range(3)]
            vel = [(vel_r if k == 0 else svel)[i] for i in range(3)]
            columns = write_blocks(k, strain, pos, vel)
            if k == 0:
                pl.semaphore_wait(bar, expected)
            send_rows(k)
            if k == 0:
                cs_v[2] = jnp.cos(angle_r[1])
                cs_v[3] = jnp.sin(angle_r[1])
                fill_picks()
                fill_weights()
            columns()
            spread_centres()
            vacc[...] = jnp.zeros((8, LANES), f32)
            for pi in (1, 2):
                rcopy(k, 1, pi).wait_recv()
            ready_row(k, jnp.int32(1), strain)
            row_pass(k, True)

            @pl.when(jnp.logical_not(first))
            def _():
                for pi in range(3):
                    rcopy(k, 0, pi).wait_recv()

            @pl.when(first)
            def _():
                for pi in range(3):
                    rcopy(k, 2, pi).wait_recv()

            ready_row(k, jnp.where(first, 2, 0), strain)
            row_pass(k, False)

            @pl.when(jnp.logical_not(edge))
            def _():
                for pi in range(3):
                    rcopy(k, 2, pi).wait_recv()
                ready_row(k, jnp.int32(2), strain)

            @pl.when(edge)
            def _():
                for d in range(NQ + 2):
                    iwait(k, d).wait_recv()
                ready_image(k, jnp.where(first, 0, 2), strain)

            row_pass(k, False)
            force = sum_forces()
            kinetic = live_v[...] * vel[0] * vel[1]
            folded = kinetic[0:8]
            for q in range(1, LP // 8):
                folded = folded + kinetic[8 * q : 8 * q + 8]
            part[F] = part[F] + folded + vacc[...] * (0.5 * DEPTH**4)
            nvx = vel[0] + DT * (force[0] - RATE * vel[1])
            nvy = vel[1] + DT * force[1]
            nvz = vel[2] + DT * force[2]
            npx = pos[0] + DT * (nvx - strain * nvy)
            npy = pos[1] + DT * nvy
            npz = pos[2] + DT * nvz
            if k == 0:
                for i, value in enumerate((npx, npy, npz)):
                    spos[i] = value
                for i, value in enumerate((nvx, nvy, nvz)):
                    svel[i] = value
            else:
                npx = npx + lax.rem(g, 2).astype(f32) + npy
                for i, value in enumerate((npx, npy, npz, nvx, nvy, nvz)):
                    comb[i, pl.ds(HP, LP), :] = value

        tail = pltpu.make_async_remote_copy(
            src_ref=comb.at[:, pl.ds(LP, HP)],
            dst_ref=comb.at[:, pl.ds(0, HP)],
            send_sem=fsem.at[0],
            recv_sem=fsem.at[1],
            device_id=(g, rt),
            device_id_type=MESH,
        )
        tail.start()

        def share(d):
            return pltpu.make_async_remote_copy(
                src_ref=part.at[F],
                dst_ref=part.at[f],
                send_sem=tsend.at[d],
                recv_sem=trecv.at[f],
                device_id=(g, lax.rem(f + d, F)),
                device_id_type=MESH,
            )

        def shared(d):
            peer = lax.rem(f + d, F)
            return pltpu.make_async_remote_copy(
                src_ref=part.at[F],
                dst_ref=part.at[peer],
                send_sem=tsend.at[d],
                recv_sem=trecv.at[peer],
                device_id=(g, peer),
                device_id_type=MESH,
            )

        for d in range(1, F):
            share(d).start()
        for k in range(2):
            finish_sends(k)
        tail.wait()
        hop = g // 2
        even = lax.rem(hop, 2) == 0
        start = HP - (hop + 1) // 2

        @pl.when(even)
        def _():
            for i in range(6):
                out = outp_r if i < 3 else outv_r
                out[i % 3] = comb[i, pl.ds(start, LP), :]

        @pl.when(jnp.logical_not(even))
        def _():
            for i in range(6):
                out = outp_r if i < 3 else outv_r
                one = pltpu.roll(comb[i, pl.ds(start, LP), :], TB, 1)
                two = pltpu.roll(comb[i, pl.ds(start + 1, LP), :], TB, 1)
                out[i % 3] = jnp.where(lowrow, one, two)

        for d in range(1, F):
            shared(d).wait_recv()
        part[f] = part[F]
        total = part[0]
        for d in range(1, F):
            total = total + part[d]
        for d in range(1, F):
            share(d).wait_send()
        whole = jnp.sum(jnp.sum(total, axis=1, keepdims=True), axis=0, keepdims=True)
        stress_r[...] = jnp.broadcast_to(whole * (-1.0 / (2.0 * NTT * 2.0 * DEPTH)), (8, LANES))

    return kernel


def per_device(G, F, bead_pos, bead_vel, noise_angle, occupancy, image_shift, strain):
    width = bead_pos.shape[2]
    LP = width // LANES
    vm = pl.BlockSpec(memory_space=pltpu.VMEM)
    sm = pl.BlockSpec(memory_space=pltpu.SMEM)
    rows = 8 * LP
    block = jax.ShapeDtypeStruct((3, LP, LANES), f32)
    dma = pltpu.SemaphoreType.DMA
    NQ = SPAN
    call = lambda branch: pl.pallas_call(
        body_of(G, F, LP, branch * NQ, NQ),
        out_shape=(block, block, jax.ShapeDtypeStruct((8, LANES), f32)),
        in_specs=[sm, sm, vm, vm, vm, vm],
        out_specs=(vm, vm, vm),
        scratch_shapes=[
            pltpu.VMEM((2, 3, LP + 2, 8, LANES), f32),
            pltpu.VMEM((F * LP, 8, LANES), f32),
            pltpu.VMEM((F * LP, 8, LANES), f32),
            pltpu.VMEM((LP * TERMS, LANES), f32),
            pltpu.VMEM((TERMS, 8 * LANES), jnp.bfloat16),
            pltpu.VMEM((LP, LANES), f32),
            pltpu.VMEM((4, LP, LANES), f32),
            pltpu.VMEM((LP, TB, 8 * LANES), f32),
            pltpu.VMEM((rows + 8, LANES), f32),
            pltpu.VMEM((rows + 8, LANES), f32),
            pltpu.VMEM((rows + 8, LANES), f32),
            pltpu.VMEM((3 * TB, LP * LANES), f32),
            pltpu.VMEM((LP * LANES, LANES), jnp.bfloat16),
            pltpu.VMEM((8, LANES), f32),
            pltpu.VMEM((3, LP, LANES), f32),
            pltpu.VMEM((3, LP, LANES), f32),
            pltpu.VMEM((6, LP + LP // 2, LANES), f32),
            pltpu.VMEM((F + 1, 8, LANES), f32),
            dma((2, 3, 3)),
            dma((2, 3, 3)),
            dma((2, NQ + 2)),
            dma((2, NQ + 2)),
            dma((2,)),
            dma((F,)),
            dma((F,)),
        ],
        compiler_params=pltpu.CompilerParams(
            collective_id=branch, has_side_effects=True, vmem_limit_bytes=48 * 1024 * 1024
        ),
    )
    args = (
        image_shift,
        strain,
        bead_pos.reshape(3, LP, LANES),
        bead_vel.reshape(3, LP, LANES),
        noise_angle.reshape(2, LP, LANES),
        occupancy,
    )
    branches = [call(branch) for branch in range(F // NQ)]
    newp, newv, stress = lax.switch(image_shift[0] // (2 * LP * NQ), branches, *args)
    shape = bead_pos.shape
    return newp.reshape(shape), newv.reshape(shape), stress[0, :1]


def solution(mesh):
    G, F = mesh.shape["grad"], mesh.shape["flow"]
    in_specs = (
        P(None, "grad", "flow"),
        P(None, "grad", "flow"),
        P(None, "grad", "flow"),
        P("grad", "flow"),
        P(),
        P(),
    )
    out_specs = (P(None, "grad", "flow"), P(None, "grad", "flow"), P("grad"))
    return jax.shard_map(
        functools.partial(per_device, G, F),
        mesh=mesh,
        in_specs=in_specs,
        out_specs=out_specs,
        check_vma=False,
    )
```

```python
import functools

import jax
import jax.numpy as jnp
from jax import lax
from jax.experimental import pallas as pl
from jax.experimental.pallas import tpu as pltpu
from jax.sharding import PartitionSpec as P

TB = 64
LANES = 128
DEPTH = TB / 6.0
INV = 6.0 / TB
REPULSION = 25.0
FRICTION = 4.5
NOISE = 15.0 * 1.4142135623730951
DT = 0.04
RATE = 0.25
FAR = 1.0e6
TERMS = 48
SPAN = 4
VSCALE = FRICTION * DEPTH**3
FSCALE = DEPTH**3
WCUT = INV * INV
MESH = pl.DeviceIdType.MESH
f32 = jnp.float32


def body_of(G, F, LP, QLO, NQ):
    NT = 2 * LP
    NTT = NT * F
    ROWS = 8 * LP
    HP = LP // 2

    def kernel(
        shift_s, strain_s, pos_r, vel_r, angle_r, occ_r,
        outp_r, outv_r, stress_r,
        rb, img0, img1, eblk, weights, live_v, cs_v, ecol, jev, jom, jop, facc, picks, vacc, spos, svel, comb, part,
        ssem, rsem, isend, irecv, fsem, tsend, trecv,
    ):
        g = lax.axis_index("grad")
        f = lax.axis_index("flow")
        up = lax.rem(g + 1, G)
        dn = lax.rem(g + G - 1, G)
        rt = lax.rem(f + 1, F)
        lf = lax.rem(f + F - 1, F)
        first = g == 0
        last = g == G - 1
        img = (img0, img1)
        lane = lax.broadcasted_iota(jnp.int32, (8, LANES), 1)
        sub = lax.broadcasted_iota(jnp.int32, (8, LANES), 0)
        low = lane < TB

        bar = pltpu.get_barrier_semaphore()

        def hello(dg, df):
            pl.semaphore_signal(bar, inc=1, device_id=(dg, df), device_id_type=MESH)

        for k in range(1, F):
            hello(g, lax.rem(f + k, F))

        @pl.when(first)
        def _():
            for k in range(F):
                hello(dn, lax.rem(f + k, F))

        @pl.when(jnp.logical_not(first))
        def _():
            for df in (lf, f, rt):
                hello(dn, df)

        @pl.when(last)
        def _():
            for k in range(F):
                hello(up, lax.rem(f + k, F))

        @pl.when(jnp.logical_not(last))
        def _():
            for df in (lf, f, rt):
                hello(up, df)

        edge = jnp.logical_or(first, last)
        expected = (F - 1) + 6 + jnp.where(edge, F - 3, 0)

        def rcopy(k, ri, pi):
            dg = (up, g, dn)[ri]
            df = (f, rt, lf)[pi]
            src = ((1, LP), (LP, 1), (1, 1))[pi]
            dst = ((1, LP), (0, 1), (LP + 1, 1))[pi]
            return pltpu.make_async_remote_copy(
                src_ref=rb.at[k, 1, pl.ds(*src)],
                dst_ref=rb.at[k, ri, pl.ds(*dst)],
                send_sem=ssem.at[k, ri, pi],
                recv_sem=rsem.at[k, ri, pi],
                device_id=(dg, df),
                device_id_type=MESH,
            )

        offs = [(d, d < 0) for d in range(-1, NQ + 1)]

        def icopy(k, d):
            hop = QLO + offs[d][0]
            df = lax.rem(f + jnp.where(first, hop, -hop) + 2 * F, F)
            dg = jnp.where(first, dn, up)
            if offs[d][1]:
                at = jnp.where(first, 0, LP - 1)
                count = 1
            else:
                at, count = 0, LP
            return pltpu.make_async_remote_copy(
                src_ref=rb.at[k, 1, pl.ds(1 + at, count)],
                dst_ref=img[k].at[pl.ds(f * LP + at, count)],
                send_sem=isend.at[k, d],
                recv_sem=irecv.at[k, d],
                device_id=(dg, df),
                device_id_type=MESH,
            )

        def iwait(k, d):
            hop = QLO + offs[d][0]
            df = lax.rem(f + jnp.where(first, hop, -hop) + 2 * F, F)
            dg = jnp.where(first, dn, up)
            if offs[d][1]:
                at = jnp.where(first, LP - 1, 0)
                count = 1
            else:
                at, count = 0, LP
            return pltpu.make_async_remote_copy(
                src_ref=rb.at[k, 1, pl.ds(1 + at, count)],
                dst_ref=img[k].at[pl.ds(df * LP + at, count)],
                send_sem=isend.at[k, d],
                recv_sem=irecv.at[k, d],
                device_id=(dg, df),
                device_id_type=MESH,
            )

        def send_rows(k):
            for pi in (1, 2):
                rcopy(k, 1, pi).start()

            @pl.when(edge)
            def _():
                for d in range(NQ + 2):
                    icopy(k, d).start()

            @pl.when(jnp.logical_not(last))
            def _():
                for pi in range(3):
                    rcopy(k, 0, pi).start()

            @pl.when(jnp.logical_not(first))
            def _():
                for pi in range(3):
                    rcopy(k, 2, pi).start()

        def finish_sends(k):
            for pi in (1, 2):
                rcopy(k, 1, pi).wait_send()

            @pl.when(edge)
            def _():
                for d in range(NQ + 2):
                    icopy(k, d).wait_send()

            @pl.when(jnp.logical_not(last))
            def _():
                for pi in range(3):
                    rcopy(k, 0, pi).wait_send()

            @pl.when(jnp.logical_not(first))
            def _():
                for pi in range(3):
                    rcopy(k, 2, pi).wait_send()

        def write_blocks(k, strain, pos, vel):
            live = live_v[...] > 0.5
            x = (pos[0] + strain * pos[1]) * INV

            def put(field, value):
                rb[k, 1, pl.ds(1, LP), field, :] = value

            def col(field, value):
                rest = value
                for term in range(3):
                    piece = rest.astype(jnp.bfloat16).astype(f32)
                    rest = rest - piece
                    for half in range(2):
                        turned = pltpu.roll(piece, TB, 1) if half else piece
                        eblk[pl.ds(term * 16 + half * 8 + field, LP, stride=TERMS), :] = turned

            y, z = pos[1] * INV, pos[2] * INV
            cosine, sine = cs_v[2 * k], cs_v[2 * k + 1]
            scaled = [vel[i] * VSCALE for i in range(3)]
            for field, value in enumerate((jnp.where(live, x, FAR), y, z, *scaled, cosine, sine)):
                put(field, value)

            def columns():
                left = (jnp.where(live, x, -FAR), y, z, *scaled, cosine * NOISE, sine * NOISE)
                for field, value in enumerate(left):
                    col(field, value)

            return columns

        def fill_weights():
            row = lax.broadcasted_iota(jnp.int32, (TERMS, 8 * LANES), 0)
            column = lax.broadcasted_iota(jnp.int32, (TERMS, 8 * LANES), 1)
            same = lax.rem(row, 16) == lax.rem(column // TB, 2) * 8 + column // LANES
            weights[...] = same.astype(f32).astype(jnp.bfloat16)

        def spread_centres():
            step = 4 if LP % 4 == 0 else 1

            def some(c, carry):
                turned = []
                for j in range(step):
                    at = pl.ds(pl.multiple_of((c * step + j) * TERMS, TERMS), TERMS)
                    turned.append(eblk[at, :].T[:TB].astype(jnp.bfloat16))
                for j in range(step):
                    ecol[c * step + j] = jnp.dot(
                        turned[j], weights[...], preferred_element_type=f32
                    )
                return carry

            lax.fori_loop(0, LP // step, some, 0)

        def offsets(strain, a, b):
            x = (2.0 * b + strain * a) * INV
            y = a * INV
            return jnp.where(sub == 0, x, jnp.where(sub == 1, y, 0.0))

        def halves(left, right):
            return jnp.where(low, pltpu.roll(left, TB, 1), pltpu.roll(right, TB, 1))

        def several(one, low_q=0, count=LP + 1):
            step = 11 if count % 11 == 0 else count

            def some(c, carry):
                for j in range(step):
                    one(low_q + c * step + j)
                return carry

            lax.fori_loop(0, count // step, some, 0)

        def ready_row(k, ri, strain, stage=None):
            a = (ri - 1).astype(f32)
            here = offsets(strain, a, 0.0)
            minus = offsets(strain, a, -1.0)
            plus = offsets(strain, a, 1.0)

            def one(q):
                now = rb[k, ri, q]
                nxt = rb[k, ri, q + 1]
                odd = halves(now, nxt)
                at = pl.ds(q * 8 if isinstance(q, int) else pl.multiple_of(q * 8, 8), 8)
                jev[at, :] = now + here
                jom[at, :] = odd + minus
                jop[at, :] = odd + plus

            if stage is None:
                several(one)
            elif stage == 0:
                several(one, 1, LP - 1)
                jev[pl.ds(8 * LP, 8), :] = rb[k, ri, LP] + here
            else:
                one(0)
                one(LP)

        def ready_image(k, ri, strain):
            a = (ri - 1).astype(f32)
            here = offsets(strain, a, 0.0)
            minus = offsets(strain, a, -1.0)
            plus = offsets(strain, a, 1.0)
            signed = shift_s[0] * (1 - 2 * lax.div(g, G - 1))

            def one(q):
                tile = lax.rem(NT * f + 2 * q - 2 + signed + 2 * NTT, NTT)
                u = lax.div(tile, 2)
                v = lax.rem(u + 1, NTT // 2)
                one_t = img[k][u]
                two_t = img[k][v]
                mixed = halves(one_t, two_t)
                is_even = jnp.broadcast_to(lax.rem(tile, 2), (8, LANES)) == 0
                now = jnp.where(is_even, one_t, mixed)
                odd = jnp.where(is_even, mixed, two_t)
                at = pl.ds(pl.multiple_of(q * 8, 8), 8)
                jev[at, :] = now + here
                jom[at, :] = odd + minus
                jop[at, :] = odd + plus

            several(one)

        def row_pass(k, fresh, pairs=None):
            count, first_p, stride = pairs or (LP, 0, 1)

            def one(n, virial):
                p = first_p + n * stride

                def partner(ref, q):
                    base = q * 8
                    return [
                        jnp.broadcast_to(ref[pl.ds(base + i, 1), :], (8, LANES))
                        for i in range(8)
                    ]

                wide = pl.ds(pl.multiple_of(p * LANES, LANES), LANES)
                sides = (partner(jom, p), partner(jev, p + 1), partner(jop, p + 1))
                for grp in range(TB // 8):
                    at = pl.ds(grp * 8, 8)
                    ex, ey, ez, eu, ev, ew, ec, es = [ecol[p, at, pl.ds(i * LANES, LANES)] for i in range(8)]
                    if fresh:
                        fx = fy = fz = jnp.zeros((8, LANES), f32)
                    else:
                        fx, fy, fz = [facc[pl.ds(i * TB + grp * 8, 8), wide] for i in range(3)]
                    for jx, jy, jz, ju, jv, jw, jc, js in sides:
                        dx = ex - jx
                        dy = ey - jy
                        dz = ez - jz
                        turn = jnp.round(dz)
                        if k > 0:
                            turn = jnp.clip(turn, -1.0, 1.0)
                        dz = dz - turn
                        w = jnp.maximum(WCUT - dx * dx - dy * dy - dz * dz, 0.0)
                        approach = dx * (eu - ju) + dy * (ev - jv) + dz * (ew - jw)
                        kick = REPULSION + (ec * jc + es * js)
                        m = w * (kick - w * approach)
                        mx = m * dx
                        fx = fx + mx
                        fy = fy + m * dy
                        fz = fz + m * dz
                        virial = virial + mx * dy
                    facc[pl.ds(0 * TB + grp * 8, 8), wide] = fx
                    facc[pl.ds(1 * TB + grp * 8, 8), wide] = fy
                    facc[pl.ds(2 * TB + grp * 8, 8), wide] = fz
                return virial

            vacc[...] = lax.fori_loop(0, count, one, vacc[...])

        lowrow = lax.broadcasted_iota(jnp.int32, (LP, LANES), 1) < TB

        def fill_picks():
            tile = lax.broadcasted_iota(jnp.int32, (LANES, LANES), 0) // TB * LP
            column = lax.broadcasted_iota(jnp.int32, (LANES, LANES), 1) - tile

            def one(p, carry):
                at = pl.ds(pl.multiple_of(p * LANES, LANES), LANES)
                picks[at, :] = (column == p).astype(f32).astype(jnp.bfloat16)
                return carry

            lax.fori_loop(0, LP, one, 0)

        def sum_forces():
            acc = facc[...]
            big = acc.astype(jnp.bfloat16)
            small = (acc - big.astype(f32)).astype(jnp.bfloat16)
            pick = picks[...]
            summed = jnp.dot(big, pick, preferred_element_type=f32)
            summed = summed + jnp.dot(small, pick, preferred_element_type=f32)
            forces = []
            for i in range(3):
                part_i = summed[i * TB : (i + 1) * TB]
                both = jnp.concatenate([part_i, part_i], axis=0).T
                forces.append(jnp.where(lowrow, both[:LP], both[LP : 2 * LP]) * FSCALE)
            return forces

        part[F] = jnp.zeros((8, LANES), f32)
        tile_of = lax.broadcasted_iota(jnp.int32, (LP, NT), 1)
        row_of = lax.broadcasted_iota(jnp.int32, (LP, NT), 0)
        counts = jnp.broadcast_to(occ_r[...].astype(f32), (LP, NT))
        counts = jnp.where(tile_of // 2 == row_of, counts, 0.0).astype(jnp.bfloat16)
        side = lax.rem(lax.broadcasted_iota(jnp.int32, (NT, LANES), 0), 2)
        half = lax.broadcasted_iota(jnp.int32, (NT, LANES), 1) // TB
        limit = jnp.dot(
            counts, (side == half).astype(f32).astype(jnp.bfloat16), preferred_element_type=f32
        )
        slot = lax.rem(lax.broadcasted_iota(jnp.int32, (LP, LANES), 1), TB).astype(f32)
        live_v[...] = (slot < limit).astype(f32)
        cs_v[0] = jnp.cos(angle_r[0])
        cs_v[1] = jnp.sin(angle_r[0])
        for k in range(2):
            strain = strain_s[0] + k * RATE * DT
            pos = [(pos_r if k == 0 else spos)[i] for i in range(3)]
            vel = [(vel_r if k == 0 else svel)[i] for i in range(3)]
            columns = write_blocks(k, strain, pos, vel)
            if k == 0:
                pl.semaphore_wait(bar, expected)
            send_rows(k)
            if k == 0:
                cs_v[2] = jnp.cos(angle_r[1])
                cs_v[3] = jnp.sin(angle_r[1])
                fill_picks()
                fill_weights()
            columns()
            spread_centres()
            vacc[...] = jnp.zeros((8, LANES), f32)
            ready_row(k, jnp.int32(1), strain, 0)
            row_pass(k, True, (LP - 2, 1, 1))
            for pi in (1, 2):
                rcopy(k, 1, pi).wait_recv()
            ready_row(k, jnp.int32(1), strain, 1)
            row_pass(k, True, (2, 0, LP - 1))

            @pl.when(jnp.logical_not(first))
            def _():
                for pi in range(3):
                    rcopy(k, 0, pi).wait_recv()

            @pl.when(first)
            def _():
                for pi in range(3):
                    rcopy(k, 2, pi).wait_recv()

            ready_row(k, jnp.where(first, 2, 0), strain)
            row_pass(k, False)

            @pl.when(jnp.logical_not(edge))
            def _():
                for pi in range(3):
                    rcopy(k, 2, pi).wait_recv()
                ready_row(k, jnp.int32(2), strain)

            @pl.when(edge)
            def _():
                for d in range(NQ + 2):
                    iwait(k, d).wait_recv()
                ready_image(k, jnp.where(first, 0, 2), strain)

            row_pass(k, False)
            force = sum_forces()
            kinetic = live_v[...] * vel[0] * vel[1]
            folded = kinetic[0:8]
            for q in range(1, LP // 8):
                folded = folded + kinetic[8 * q : 8 * q + 8]
            part[F] = part[F] + folded + vacc[...] * (0.5 * DEPTH**4)
            nvx = vel[0] + DT * (force[0] - RATE * vel[1])
            nvy = vel[1] + DT * force[1]
            nvz = vel[2] + DT * force[2]
            npx = pos[0] + DT * (nvx - strain * nvy)
            npy = pos[1] + DT * nvy
            npz = pos[2] + DT * nvz
            if k == 0:
                for i, value in enumerate((npx, npy, npz)):
                    spos[i] = value
                for i, value in enumerate((nvx, nvy, nvz)):
                    svel[i] = value
            else:
                npx = npx + lax.rem(g, 2).astype(f32) + npy
                for i, value in enumerate((npx, npy, npz, nvx, nvy, nvz)):
                    comb[i, pl.ds(HP, LP), :] = value

        tail = pltpu.make_async_remote_copy(
            src_ref=comb.at[:, pl.ds(LP, HP)],
            dst_ref=comb.at[:, pl.ds(0, HP)],
            send_sem=fsem.at[0],
            recv_sem=fsem.at[1],
            device_id=(g, rt),
            device_id_type=MESH,
        )
        tail.start()

        def share(d):
            return pltpu.make_async_remote_copy(
                src_ref=part.at[F],
                dst_ref=part.at[f],
                send_sem=tsend.at[d],
                recv_sem=trecv.at[f],
                device_id=(g, lax.rem(f + d, F)),
                device_id_type=MESH,
            )

        def shared(d):
            peer = lax.rem(f + d, F)
            return pltpu.make_async_remote_copy(
                src_ref=part.at[F],
                dst_ref=part.at[peer],
                send_sem=tsend.at[d],
                recv_sem=trecv.at[peer],
                device_id=(g, peer),
                device_id_type=MESH,
            )

        for d in range(1, F):
            share(d).start()
        for k in range(2):
            finish_sends(k)
        tail.wait()
        hop = g // 2
        even = lax.rem(hop, 2) == 0
        start = HP - (hop + 1) // 2

        @pl.when(even)
        def _():
            for i in range(6):
                out = outp_r if i < 3 else outv_r
                out[i % 3] = comb[i, pl.ds(start, LP), :]

        @pl.when(jnp.logical_not(even))
        def _():
            for i in range(6):
                out = outp_r if i < 3 else outv_r
                one = pltpu.roll(comb[i, pl.ds(start, LP), :], TB, 1)
                two = pltpu.roll(comb[i, pl.ds(start + 1, LP), :], TB, 1)
                out[i % 3] = jnp.where(lowrow, one, two)

        for d in range(1, F):
            shared(d).wait_recv()
        part[f] = part[F]
        total = part[0]
        for d in range(1, F):
            total = total + part[d]
        for d in range(1, F):
            share(d).wait_send()
        whole = jnp.sum(jnp.sum(total, axis=1, keepdims=True), axis=0, keepdims=True)
        stress_r[...] = jnp.broadcast_to(whole * (-1.0 / (2.0 * NTT * 2.0 * DEPTH)), (8, LANES))

    return kernel


def per_device(G, F, bead_pos, bead_vel, noise_angle, occupancy, image_shift, strain):
    width = bead_pos.shape[2]
    LP = width // LANES
    vm = pl.BlockSpec(memory_space=pltpu.VMEM)
    sm = pl.BlockSpec(memory_space=pltpu.SMEM)
    rows = 8 * LP
    block = jax.ShapeDtypeStruct((3, LP, LANES), f32)
    dma = pltpu.SemaphoreType.DMA
    NQ = SPAN
    call = lambda branch: pl.pallas_call(
        body_of(G, F, LP, branch * NQ, NQ),
        out_shape=(block, block, jax.ShapeDtypeStruct((8, LANES), f32)),
        in_specs=[sm, sm, vm, vm, vm, vm],
        out_specs=(vm, vm, vm),
        scratch_shapes=[
            pltpu.VMEM((2, 3, LP + 2, 8, LANES), f32),
            pltpu.VMEM((F * LP, 8, LANES), f32),
            pltpu.VMEM((F * LP, 8, LANES), f32),
            pltpu.VMEM((LP * TERMS, LANES), f32),
            pltpu.VMEM((TERMS, 8 * LANES), jnp.bfloat16),
            pltpu.VMEM((LP, LANES), f32),
            pltpu.VMEM((4, LP, LANES), f32),
            pltpu.VMEM((LP, TB, 8 * LANES), f32),
            pltpu.VMEM((rows + 8, LANES), f32),
            pltpu.VMEM((rows + 8, LANES), f32),
            pltpu.VMEM((rows + 8, LANES), f32),
            pltpu.VMEM((3 * TB, LP * LANES), f32),
            pltpu.VMEM((LP * LANES, LANES), jnp.bfloat16),
            pltpu.VMEM((8, LANES), f32),
            pltpu.VMEM((3, LP, LANES), f32),
            pltpu.VMEM((3, LP, LANES), f32),
            pltpu.VMEM((6, LP + LP // 2, LANES), f32),
            pltpu.VMEM((F + 1, 8, LANES), f32),
            dma((2, 3, 3)),
            dma((2, 3, 3)),
            dma((2, NQ + 2)),
            dma((2, NQ + 2)),
            dma((2,)),
            dma((F,)),
            dma((F,)),
        ],
        compiler_params=pltpu.CompilerParams(
            collective_id=branch, has_side_effects=True, vmem_limit_bytes=48 * 1024 * 1024
        ),
    )
    args = (
        image_shift,
        strain,
        bead_pos.reshape(3, LP, LANES),
        bead_vel.reshape(3, LP, LANES),
        noise_angle.reshape(2, LP, LANES),
        occupancy,
    )
    branches = [call(branch) for branch in range(F // NQ)]
    newp, newv, stress = lax.switch(image_shift[0] // (2 * LP * NQ), branches, *args)
    shape = bead_pos.shape
    return newp.reshape(shape), newv.reshape(shape), stress[0, :1]


def solution(mesh):
    G, F = mesh.shape["grad"], mesh.shape["flow"]
    in_specs = (
        P(None, "grad", "flow"),
        P(None, "grad", "flow"),
        P(None, "grad", "flow"),
        P("grad", "flow"),
        P(),
        P(),
    )
    out_specs = (P(None, "grad", "flow"), P(None, "grad", "flow"), P("grad"))
    return jax.shard_map(
        functools.partial(per_device, G, F),
        mesh=mesh,
        in_specs=in_specs,
        out_specs=out_specs,
        check_vma=False,
    )
```

```python
import functools

import jax
import jax.numpy as jnp
from jax import lax
from jax.experimental import pallas as pl
from jax.experimental.pallas import tpu as pltpu
from jax.sharding import PartitionSpec as P

TB = 64
LANES = 128
DEPTH = TB / 6.0
INV = 6.0 / TB
REPULSION = 25.0
FRICTION = 4.5
NOISE = 15.0 * 1.4142135623730951
DT = 0.04
RATE = 0.25
FAR = 1.0e6
TERMS = 48
SPAN = 4
VSCALE = FRICTION * DEPTH**3
FSCALE = DEPTH**3
WCUT = INV * INV
MESH = pl.DeviceIdType.MESH
f32 = jnp.float32


def body_of(G, F, LP, QLO, NQ):
    NT = 2 * LP
    NTT = NT * F
    ROWS = 8 * LP
    HP = LP // 2

    def kernel(
        shift_s, strain_s, pos_r, vel_r, angle_r, occ_r,
        outp_r, outv_r, stress_r,
        rb, img0, img1, eblk, weights, live_v, cs_v, ecol, jev, jom, jop, facc, picks, vacc, spos, svel, comb, part,
        ssem, rsem, isend, irecv, fsem, tsend, trecv,
    ):
        g = lax.axis_index("grad")
        f = lax.axis_index("flow")
        up = lax.rem(g + 1, G)
        dn = lax.rem(g + G - 1, G)
        rt = lax.rem(f + 1, F)
        lf = lax.rem(f + F - 1, F)
        first = g == 0
        last = g == G - 1
        img = (img0, img1)
        lane = lax.broadcasted_iota(jnp.int32, (8, LANES), 1)
        sub = lax.broadcasted_iota(jnp.int32, (8, LANES), 0)
        low = lane < TB

        bar = pltpu.get_barrier_semaphore()

        def hello(dg, df):
            pl.semaphore_signal(bar, inc=1, device_id=(dg, df), device_id_type=MESH)

        for k in range(1, F):
            hello(g, lax.rem(f + k, F))

        @pl.when(first)
        def _():
            for k in range(F):
                hello(dn, lax.rem(f + k, F))

        @pl.when(jnp.logical_not(first))
        def _():
            for df in (lf, f, rt):
                hello(dn, df)

        @pl.when(last)
        def _():
            for k in range(F):
                hello(up, lax.rem(f + k, F))

        @pl.when(jnp.logical_not(last))
        def _():
            for df in (lf, f, rt):
                hello(up, df)

        edge = jnp.logical_or(first, last)
        expected = (F - 1) + 6 + jnp.where(edge, F - 3, 0)

        def rcopy(k, ri, pi):
            dg = (up, g, dn)[ri]
            df = (f, rt, lf)[pi]
            src = ((1, LP), (LP, 1), (1, 1))[pi]
            dst = ((1, LP), (0, 1), (LP + 1, 1))[pi]
            return pltpu.make_async_remote_copy(
                src_ref=rb.at[k, 1, pl.ds(*src)],
                dst_ref=rb.at[k, ri, pl.ds(*dst)],
                send_sem=ssem.at[k, ri, pi],
                recv_sem=rsem.at[k, ri, pi],
                device_id=(dg, df),
                device_id_type=MESH,
            )

        offs = [(d, d < 0) for d in range(-1, NQ + 1)]

        def icopy(k, d):
            hop = QLO + offs[d][0]
            df = lax.rem(f + jnp.where(first, hop, -hop) + 2 * F, F)
            dg = jnp.where(first, dn, up)
            if offs[d][1]:
                at = jnp.where(first, 0, LP - 1)
                count = 1
            else:
                at, count = 0, LP
            return pltpu.make_async_remote_copy(
                src_ref=rb.at[k, 1, pl.ds(1 + at, count)],
                dst_ref=img[k].at[pl.ds(f * LP + at, count)],
                send_sem=isend.at[k, d],
                recv_sem=irecv.at[k, d],
                device_id=(dg, df),
                device_id_type=MESH,
            )

        def iwait(k, d):
            hop = QLO + offs[d][0]
            df = lax.rem(f + jnp.where(first, hop, -hop) + 2 * F, F)
            dg = jnp.where(first, dn, up)
            if offs[d][1]:
                at = jnp.where(first, LP - 1, 0)
                count = 1
            else:
                at, count = 0, LP
            return pltpu.make_async_remote_copy(
                src_ref=rb.at[k, 1, pl.ds(1 + at, count)],
                dst_ref=img[k].at[pl.ds(df * LP + at, count)],
                send_sem=isend.at[k, d],
                recv_sem=irecv.at[k, d],
                device_id=(dg, df),
                device_id_type=MESH,
            )

        def send_rows(k):
            for pi in (1, 2):
                rcopy(k, 1, pi).start()

            @pl.when(edge)
            def _():
                for d in range(NQ + 2):
                    icopy(k, d).start()

            @pl.when(jnp.logical_not(last))
            def _():
                for pi in range(3):
                    rcopy(k, 0, pi).start()

            @pl.when(jnp.logical_not(first))
            def _():
                for pi in range(3):
                    rcopy(k, 2, pi).start()

        def finish_sends(k):
            for pi in (1, 2):
                rcopy(k, 1, pi).wait_send()

            @pl.when(edge)
            def _():
                for d in range(NQ + 2):
                    icopy(k, d).wait_send()

            @pl.when(jnp.logical_not(last))
            def _():
                for pi in range(3):
                    rcopy(k, 0, pi).wait_send()

            @pl.when(jnp.logical_not(first))
            def _():
                for pi in range(3):
                    rcopy(k, 2, pi).wait_send()

        def write_blocks(k, strain, pos, vel):
            live = live_v[...] > 0.5
            x = (pos[0] + strain * pos[1]) * INV

            def put(field, value):
                rb[k, 1, pl.ds(1, LP), field, :] = value

            def col(field, value):
                rest = value
                for term in range(3):
                    piece = rest.astype(jnp.bfloat16).astype(f32)
                    rest = rest - piece
                    for half in range(2):
                        turned = pltpu.roll(piece, TB, 1) if half else piece
                        eblk[pl.ds(term * 16 + half * 8 + field, LP, stride=TERMS), :] = turned

            y, z = pos[1] * INV, pos[2] * INV
            cosine, sine = cs_v[2 * k], cs_v[2 * k + 1]
            scaled = [vel[i] * VSCALE for i in range(3)]
            for field, value in enumerate((jnp.where(live, x, FAR), y, z, *scaled, cosine, sine)):
                put(field, value)

            def columns():
                left = (jnp.where(live, x, -FAR), y, z, *scaled, cosine * NOISE, sine * NOISE)
                for field, value in enumerate(left):
                    col(field, value)

            return columns

        def fill_weights():
            row = lax.broadcasted_iota(jnp.int32, (TERMS, 8 * LANES), 0)
            column = lax.broadcasted_iota(jnp.int32, (TERMS, 8 * LANES), 1)
            same = lax.rem(row, 16) == lax.rem(column // TB, 2) * 8 + column // LANES
            weights[...] = same.astype(f32).astype(jnp.bfloat16)

        def spread_centres():
            step = 8 if LP % 8 == 0 else 1

            def some(c, carry):
                turned = []
                for j in range(step):
                    at = pl.ds(pl.multiple_of((c * step + j) * TERMS, TERMS), TERMS)
                    turned.append(eblk[at, :].T[:TB].astype(jnp.bfloat16))
                for j in range(step):
                    ecol[c * step + j] = jnp.dot(
                        turned[j], weights[...], preferred_element_type=f32
                    )
                return carry

            lax.fori_loop(0, LP // step, some, 0)

        def offsets(strain, a, b):
            x = (2.0 * b + strain * a) * INV
            y = a * INV
            return jnp.where(sub == 0, x, jnp.where(sub == 1, y, 0.0))

        def halves(left, right):
            return jnp.where(low, pltpu.roll(left, TB, 1), pltpu.roll(right, TB, 1))

        def several(one, low_q=0, count=LP + 1):
            step = 11 if count % 11 == 0 else count

            def some(c, carry):
                for j in range(step):
                    one(low_q + c * step + j)
                return carry

            lax.fori_loop(0, count // step, some, 0)

        def ready_row(k, ri, strain, stage=None):
            a = (ri - 1).astype(f32)
            here = offsets(strain, a, 0.0)
            minus = offsets(strain, a, -1.0)
            plus = offsets(strain, a, 1.0)

            def one(q):
                now = rb[k, ri, q]
                nxt = rb[k, ri, q + 1]
                odd = halves(now, nxt)
                at = pl.ds(q * 8 if isinstance(q, int) else pl.multiple_of(q * 8, 8), 8)
                jev[at, :] = now + here
                jom[at, :] = odd + minus
                jop[at, :] = odd + plus

            if stage is None:
                several(one)
            elif stage == 0:
                several(one, 1, LP - 1)
                jev[pl.ds(8 * LP, 8), :] = rb[k, ri, LP] + here
            else:
                one(0)
                one(LP)

        def ready_image(k, ri, strain):
            a = (ri - 1).astype(f32)
            here = offsets(strain, a, 0.0)
            minus = offsets(strain, a, -1.0)
            plus = offsets(strain, a, 1.0)
            signed = shift_s[0] * (1 - 2 * lax.div(g, G - 1))

            def one(q):
                tile = lax.rem(NT * f + 2 * q - 2 + signed + 2 * NTT, NTT)
                u = lax.div(tile, 2)
                v = lax.rem(u + 1, NTT // 2)
                one_t = img[k][u]
                two_t = img[k][v]
                mixed = halves(one_t, two_t)
                is_even = jnp.broadcast_to(lax.rem(tile, 2), (8, LANES)) == 0
                now = jnp.where(is_even, one_t, mixed)
                odd = jnp.where(is_even, mixed, two_t)
                at = pl.ds(pl.multiple_of(q * 8, 8), 8)
                jev[at, :] = now + here
                jom[at, :] = odd + minus
                jop[at, :] = odd + plus

            several(one)

        def row_pass(k, fresh, pairs=None):
            count, first_p, stride = pairs or (LP, 0, 1)

            def one(n, virial):
                p = first_p + n * stride

                def partner(ref, q):
                    base = q * 8
                    return [
                        jnp.broadcast_to(ref[pl.ds(base + i, 1), :], (8, LANES))
                        for i in range(8)
                    ]

                wide = pl.ds(pl.multiple_of(p * LANES, LANES), LANES)
                sides = (partner(jom, p), partner(jev, p + 1), partner(jop, p + 1))
                for grp in range(TB // 8):
                    at = pl.ds(grp * 8, 8)
                    ex, ey, ez, eu, ev, ew, ec, es = [ecol[p, at, pl.ds(i * LANES, LANES)] for i in range(8)]
                    if fresh:
                        fx = fy = fz = jnp.zeros((8, LANES), f32)
                    else:
                        fx, fy, fz = [facc[pl.ds(i * TB + grp * 8, 8), wide] for i in range(3)]
                    for jx, jy, jz, ju, jv, jw, jc, js in sides:
                        dx = ex - jx
                        dy = ey - jy
                        dz = ez - jz
                        turn = jnp.round(dz)
                        if k > 0:
                            turn = jnp.clip(turn, -1.0, 1.0)
                        dz = dz - turn
                        w = jnp.maximum(WCUT - dx * dx - dy * dy - dz * dz, 0.0)
                        approach = dx * (eu - ju) + dy * (ev - jv) + dz * (ew - jw)
                        kick = REPULSION + (ec * jc + es * js)
                        m = w * (kick - w * approach)
                        mx = m * dx
                        fx = fx + mx
                        fy = fy + m * dy
                        fz = fz + m * dz
                        if not fresh:
                            virial = virial + mx * dy
                    if fresh:
                        virial = virial + ey * (fx + fx)
                    facc[pl.ds(0 * TB + grp * 8, 8), wide] = fx
                    facc[pl.ds(1 * TB + grp * 8, 8), wide] = fy
                    facc[pl.ds(2 * TB + grp * 8, 8), wide] = fz
                return virial

            vacc[...] = lax.fori_loop(0, count, one, vacc[...])

        lowrow = lax.broadcasted_iota(jnp.int32, (LP, LANES), 1) < TB

        def fill_picks():
            tile = lax.broadcasted_iota(jnp.int32, (LANES, LANES), 0) // TB * LP
            column = lax.broadcasted_iota(jnp.int32, (LANES, LANES), 1) - tile

            def one(p, carry):
                at = pl.ds(pl.multiple_of(p * LANES, LANES), LANES)
                picks[at, :] = (column == p).astype(f32).astype(jnp.bfloat16)
                return carry

            lax.fori_loop(0, LP, one, 0)

        def sum_forces():
            acc = facc[...]
            big = acc.astype(jnp.bfloat16)
            small = (acc - big.astype(f32)).astype(jnp.bfloat16)
            pick = picks[...]
            summed = jnp.dot(big, pick, preferred_element_type=f32)
            summed = summed + jnp.dot(small, pick, preferred_element_type=f32)
            forces = []
            for i in range(3):
                part_i = summed[i * TB : (i + 1) * TB]
                both = jnp.concatenate([part_i, part_i], axis=0).T
                forces.append(jnp.where(lowrow, both[:LP], both[LP : 2 * LP]) * FSCALE)
            return forces

        part[F] = jnp.zeros((8, LANES), f32)
        tile_of = lax.broadcasted_iota(jnp.int32, (LP, NT), 1)
        row_of = lax.broadcasted_iota(jnp.int32, (LP, NT), 0)
        counts = jnp.broadcast_to(occ_r[...].astype(f32), (LP, NT))
        counts = jnp.where(tile_of // 2 == row_of, counts, 0.0).astype(jnp.bfloat16)
        side = lax.rem(lax.broadcasted_iota(jnp.int32, (NT, LANES), 0), 2)
        half = lax.broadcasted_iota(jnp.int32, (NT, LANES), 1) // TB
        limit = jnp.dot(
            counts, (side == half).astype(f32).astype(jnp.bfloat16), preferred_element_type=f32
        )
        slot = lax.rem(lax.broadcasted_iota(jnp.int32, (LP, LANES), 1), TB).astype(f32)
        live_v[...] = (slot < limit).astype(f32)
        cs_v[0] = jnp.cos(angle_r[0])
        cs_v[1] = jnp.sin(angle_r[0])
        for k in range(2):
            strain = strain_s[0] + k * RATE * DT
            pos = [(pos_r if k == 0 else spos)[i] for i in range(3)]
            vel = [(vel_r if k == 0 else svel)[i] for i in range(3)]
            columns = write_blocks(k, strain, pos, vel)
            if k == 0:
                pl.semaphore_wait(bar, expected)
            send_rows(k)
            if k == 0:
                cs_v[2] = jnp.cos(angle_r[1])
                cs_v[3] = jnp.sin(angle_r[1])
                fill_picks()
                fill_weights()
            columns()
            spread_centres()
            vacc[...] = jnp.zeros((8, LANES), f32)
            ready_row(k, jnp.int32(1), strain, 0)
            row_pass(k, True, (LP - 2, 1, 1))
            for pi in (1, 2):
                rcopy(k, 1, pi).wait_recv()
            ready_row(k, jnp.int32(1), strain, 1)
            row_pass(k, True, (2, 0, LP - 1))

            @pl.when(jnp.logical_not(first))
            def _():
                for pi in range(3):
                    rcopy(k, 0, pi).wait_recv()

            @pl.when(first)
            def _():
                for pi in range(3):
                    rcopy(k, 2, pi).wait_recv()

            ready_row(k, jnp.where(first, 2, 0), strain)
            row_pass(k, False)

            @pl.when(jnp.logical_not(edge))
            def _():
                for pi in range(3):
                    rcopy(k, 2, pi).wait_recv()
                ready_row(k, jnp.int32(2), strain)

            @pl.when(edge)
            def _():
                for d in range(NQ + 2):
                    iwait(k, d).wait_recv()
                ready_image(k, jnp.where(first, 0, 2), strain)

            row_pass(k, False)
            force = sum_forces()
            kinetic = live_v[...] * vel[0] * vel[1]
            folded = kinetic[0:8]
            for q in range(1, LP // 8):
                folded = folded + kinetic[8 * q : 8 * q + 8]
            part[F] = part[F] + folded + vacc[...] * (0.5 * DEPTH**4)
            nvx = vel[0] + DT * (force[0] - RATE * vel[1])
            nvy = vel[1] + DT * force[1]
            nvz = vel[2] + DT * force[2]
            npx = pos[0] + DT * (nvx - strain * nvy)
            npy = pos[1] + DT * nvy
            npz = pos[2] + DT * nvz
            if k == 0:
                for i, value in enumerate((npx, npy, npz)):
                    spos[i] = value
                for i, value in enumerate((nvx, nvy, nvz)):
                    svel[i] = value
            else:
                npx = npx + lax.rem(g, 2).astype(f32) + npy
                for i, value in enumerate((npx, npy, npz, nvx, nvy, nvz)):
                    comb[i, pl.ds(HP, LP), :] = value

        tail = pltpu.make_async_remote_copy(
            src_ref=comb.at[:, pl.ds(LP, HP)],
            dst_ref=comb.at[:, pl.ds(0, HP)],
            send_sem=fsem.at[0],
            recv_sem=fsem.at[1],
            device_id=(g, rt),
            device_id_type=MESH,
        )
        tail.start()

        def share(d):
            return pltpu.make_async_remote_copy(
                src_ref=part.at[F],
                dst_ref=part.at[f],
                send_sem=tsend.at[d],
                recv_sem=trecv.at[f],
                device_id=(g, lax.rem(f + d, F)),
                device_id_type=MESH,
            )

        def shared(d):
            peer = lax.rem(f + d, F)
            return pltpu.make_async_remote_copy(
                src_ref=part.at[F],
                dst_ref=part.at[peer],
                send_sem=tsend.at[d],
                recv_sem=trecv.at[peer],
                device_id=(g, peer),
                device_id_type=MESH,
            )

        for d in range(1, F):
            share(d).start()
        for k in range(2):
            finish_sends(k)
        tail.wait()
        hop = g // 2
        even = lax.rem(hop, 2) == 0
        start = HP - (hop + 1) // 2

        @pl.when(even)
        def _():
            for i in range(6):
                out = outp_r if i < 3 else outv_r
                out[i % 3] = comb[i, pl.ds(start, LP), :]

        @pl.when(jnp.logical_not(even))
        def _():
            for i in range(6):
                out = outp_r if i < 3 else outv_r
                one = pltpu.roll(comb[i, pl.ds(start, LP), :], TB, 1)
                two = pltpu.roll(comb[i, pl.ds(start + 1, LP), :], TB, 1)
                out[i % 3] = jnp.where(lowrow, one, two)

        for d in range(1, F):
            shared(d).wait_recv()
        part[f] = part[F]
        total = part[0]
        for d in range(1, F):
            total = total + part[d]
        for d in range(1, F):
            share(d).wait_send()
        whole = jnp.sum(jnp.sum(total, axis=1, keepdims=True), axis=0, keepdims=True)
        stress_r[...] = jnp.broadcast_to(whole * (-1.0 / (2.0 * NTT * 2.0 * DEPTH)), (8, LANES))

    return kernel


def per_device(G, F, bead_pos, bead_vel, noise_angle, occupancy, image_shift, strain):
    width = bead_pos.shape[2]
    LP = width // LANES
    vm = pl.BlockSpec(memory_space=pltpu.VMEM)
    sm = pl.BlockSpec(memory_space=pltpu.SMEM)
    rows = 8 * LP
    block = jax.ShapeDtypeStruct((3, LP, LANES), f32)
    dma = pltpu.SemaphoreType.DMA
    NQ = SPAN
    call = lambda branch: pl.pallas_call(
        body_of(G, F, LP, branch * NQ, NQ),
        out_shape=(block, block, jax.ShapeDtypeStruct((8, LANES), f32)),
        in_specs=[sm, sm, vm, vm, vm, vm],
        out_specs=(vm, vm, vm),
        scratch_shapes=[
            pltpu.VMEM((2, 3, LP + 2, 8, LANES), f32),
            pltpu.VMEM((F * LP, 8, LANES), f32),
            pltpu.VMEM((F * LP, 8, LANES), f32),
            pltpu.VMEM((LP * TERMS, LANES), f32),
            pltpu.VMEM((TERMS, 8 * LANES), jnp.bfloat16),
            pltpu.VMEM((LP, LANES), f32),
            pltpu.VMEM((4, LP, LANES), f32),
            pltpu.VMEM((LP, TB, 8 * LANES), f32),
            pltpu.VMEM((rows + 8, LANES), f32),
            pltpu.VMEM((rows + 8, LANES), f32),
            pltpu.VMEM((rows + 8, LANES), f32),
            pltpu.VMEM((3 * TB, LP * LANES), f32),
            pltpu.VMEM((LP * LANES, LANES), jnp.bfloat16),
            pltpu.VMEM((8, LANES), f32),
            pltpu.VMEM((3, LP, LANES), f32),
            pltpu.VMEM((3, LP, LANES), f32),
            pltpu.VMEM((6, LP + LP // 2, LANES), f32),
            pltpu.VMEM((F + 1, 8, LANES), f32),
            dma((2, 3, 3)),
            dma((2, 3, 3)),
            dma((2, NQ + 2)),
            dma((2, NQ + 2)),
            dma((2,)),
            dma((F,)),
            dma((F,)),
        ],
        compiler_params=pltpu.CompilerParams(
            collective_id=branch, has_side_effects=True, vmem_limit_bytes=48 * 1024 * 1024
        ),
    )
    args = (
        image_shift,
        strain,
        bead_pos.reshape(3, LP, LANES),
        bead_vel.reshape(3, LP, LANES),
        noise_angle.reshape(2, LP, LANES),
        occupancy,
    )
    branches = [call(branch) for branch in range(F // NQ)]
    newp, newv, stress = lax.switch(image_shift[0] // (2 * LP * NQ), branches, *args)
    shape = bead_pos.shape
    return newp.reshape(shape), newv.reshape(shape), stress[0, :1]


def solution(mesh):
    G, F = mesh.shape["grad"], mesh.shape["flow"]
    in_specs = (
        P(None, "grad", "flow"),
        P(None, "grad", "flow"),
        P(None, "grad", "flow"),
        P("grad", "flow"),
        P(),
        P(),
    )
    out_specs = (P(None, "grad", "flow"), P(None, "grad", "flow"), P("grad"))
    return jax.shard_map(
        functools.partial(per_device, G, F),
        mesh=mesh,
        in_specs=in_specs,
        out_specs=out_specs,
        check_vma=False,
    )
```
